32 devices in a mesh: ez: 4 (over z), ey: 2 (over y), ex: 4 (over x, core).
Axes of the slice: x: 2, y: 2, z: 4, core: 2. Of those that a mesh axis runs over, the one named last changes fastest.
Arguments:
- tokens_in: bfloat16 [2, 8192, 1536], P(None, ('ez', 'ey', 'ex'))
- expert_ids: int32 [2, 2, 8192, 6], P(None, None, ('ez', 'ey', 'ex'))
- gate_vals: float32 [2, 2, 8192, 6], P(None, None, ('ez', 'ey', 'ex'))
- w_up1: bfloat16 [2, 64, 1536, 512], P(None, ('ez', 'ey', 'ex'))
- w_up3: bfloat16 [2, 64, 1536, 512], P(None, ('ez', 'ey', 'ex'))
- w_down: bfloat16 [2, 64, 512, 1536], P(None, ('ez', 'ey', 'ex'))
Outputs:
- output: bfloat16 [2, 8192, 1536], P(None, ('ez', 'ey', 'ex'))
All inputs are finite; a program needn't handle non-finite values.
Results may differ from the reference program's by a relative error of at most 0.0115358.
Values are sent between devices in bfloat16 or wider.
A program may use at most 1 GiB of HBM per device.

```python
import jax
import jax.numpy as jnp
import numpy as np
from jax import lax

HIDDEN = 1536
FFN_DIM = 512
EXPERTS = 64
TOP_K = 6
TOK_MB = 256
DEVICES = 32
LAYERS = 2
MICRO_BATCHES = 2
CAPACITY = 2 * ((TOK_MB * TOP_K + EXPERTS - 1) // EXPERTS)
ROWS_MAX = DEVICES * CAPACITY
ROUTE_SCALE = 2.5


def rank_table():
    hot_count = EXPERTS // 16 + 1
    rest_total = TOK_MB * TOP_K - hot_count * CAPACITY
    cold_count = EXPERTS - hot_count
    base_share = rest_total // cold_count
    extra_count = rest_total % cold_count
    counts = [CAPACITY] * hot_count + [base_share + 1] * extra_count + [base_share] * (cold_count - extra_count)
    return np.repeat(np.arange(EXPERTS), counts).reshape(TOP_K, TOK_MB).T.astype(np.int32)


def route_block(key):
    key_perm, key_tok, key_roll = jax.random.split(key, 3)
    expert_perm = jax.random.permutation(key_perm, EXPERTS)
    chosen = expert_perm[jnp.asarray(rank_table())]
    chosen = chosen[jax.random.permutation(key_tok, TOK_MB)]
    roll_shift = jax.random.randint(key_roll, (TOK_MB, 1), 0, TOP_K)
    slot_order = (jnp.arange(TOP_K)[None, :] + roll_shift) % TOP_K
    return jnp.take_along_axis(chosen, slot_order, axis=1).astype(jnp.int32)


def setup_inputs(seed: int = 0) -> dict:
    key = jax.random.key(seed)
    key_x, key_ids, key_gate, key_up1, key_up3, key_down = jax.random.split(key, 6)
    n_tokens = DEVICES * TOK_MB
    tokens_in = jax.random.normal(key_x, (MICRO_BATCHES, n_tokens, HIDDEN), jnp.float32).astype(jnp.bfloat16)
    block_keys = jax.random.split(key_ids, LAYERS * MICRO_BATCHES * DEVICES)
    expert_ids = jax.vmap(route_block)(block_keys).reshape(LAYERS, MICRO_BATCHES, n_tokens, TOP_K)
    raw_gates = jax.random.uniform(key_gate, (LAYERS, MICRO_BATCHES, n_tokens, TOP_K), jnp.float32, 0.25, 1.75)
    gate_vals = raw_gates / jnp.sum(raw_gates, axis=-1, keepdims=True)
    up_shape = (LAYERS, EXPERTS, HIDDEN, FFN_DIM)
    w_up1 = (jax.random.normal(key_up1, up_shape, jnp.float32) * HIDDEN ** -0.5).astype(jnp.bfloat16)
    w_up3 = (jax.random.normal(key_up3, up_shape, jnp.float32) * HIDDEN ** -0.5).astype(jnp.bfloat16)
    w_down = (jax.random.normal(key_down, (LAYERS, EXPERTS, FFN_DIM, HIDDEN), jnp.float32) * FFN_DIM ** -0.5).astype(jnp.bfloat16)
    return {"tokens_in": tokens_in, "expert_ids": expert_ids, "gate_vals": gate_vals, "w_up1": w_up1, "w_up3": w_up3, "w_down": w_down}


def moe_layer(tokens, ids_mb, gates_mb, mat_up1, mat_up3, mat_down):
    n_assign = tokens.shape[0] * TOP_K
    flat_ids = ids_mb.reshape(n_assign)
    sort_order = jnp.argsort(flat_ids, stable=True)
    counts = jnp.bincount(flat_ids, length=EXPERTS)
    starts = jnp.cumsum(counts) - counts
    row_pos = jnp.arange(ROWS_MAX)

    def one_expert(operands):
        first_row, row_count, mat_a, mat_b, mat_c = operands
        picked = sort_order[jnp.minimum(first_row + row_pos, n_assign - 1)]
        expert_rows = tokens[picked // TOP_K]
        gate_in = jnp.dot(expert_rows, mat_a, preferred_element_type=jnp.float32)
        lin_in = jnp.dot(expert_rows, mat_b, preferred_element_type=jnp.float32)
        hidden = (jax.nn.silu(gate_in) * lin_in).astype(jnp.bfloat16)
        expert_out = jnp.dot(hidden, mat_c, preferred_element_type=jnp.float32).astype(jnp.bfloat16)
        return expert_out, jnp.where(row_pos < row_count, picked, n_assign)

    all_out, targets = lax.map(one_expert, (starts, counts, mat_up1, mat_up3, mat_down))
    per_assign = jnp.zeros((n_assign + 1, HIDDEN), jnp.bfloat16).at[targets.reshape(-1)].set(all_out.reshape(-1, HIDDEN))
    per_assign = per_assign[:n_assign].reshape(tokens.shape[0], TOP_K, HIDDEN)
    moe_sum = jnp.einsum("tj,tjh->th", gates_mb.astype(jnp.float32), per_assign.astype(jnp.float32))
    return (tokens.astype(jnp.float32) + ROUTE_SCALE * moe_sum).astype(jnp.bfloat16)


def reference(tokens_in, expert_ids, gate_vals, w_up1, w_up3, w_down):
    def layer_step(layer_in, layer_args):
        ids_layer, gates_layer, mat_up1, mat_up3, mat_down = layer_args

        def one_batch(batch_args):
            batch_tok, ids_mb, gates_mb = batch_args
            return moe_layer(batch_tok, ids_mb, gates_mb, mat_up1, mat_up3, mat_down)

        return lax.map(one_batch, (layer_in, ids_layer, gates_layer)), None

    tokens_out, _ = lax.scan(layer_step, tokens_in, (expert_ids, gate_vals, w_up1, w_up3, w_down))
    return tokens_out
```

```python
import functools

import jax
import jax.numpy as jnp
from jax import lax
from jax.experimental import pallas as pl
from jax.experimental.pallas import tpu as pltpu
from jax.sharding import PartitionSpec as P

ROUTE_SCALE = 2.5
MESH_AXES = ("ez", "ey", "ex")
PLANE_AXES = ("ey", "ex")


def capacity_of(tok_mb, top_k, experts):
    return 2 * ((tok_mb * top_k + experts - 1) // experts)


def slot_table(ids, experts, capacity):
    chosen = (ids[..., None] == jnp.arange(experts)).astype(jnp.int32)
    per_expert = jnp.sum(chosen, axis=-2)
    token_rank = jnp.cumsum(per_expert, axis=-2) - per_expert
    slot_pos = jnp.sum(chosen * token_rank[..., None, :], axis=-1)
    return ids * capacity + slot_pos


def dispatch_kernel(slots_ref, tok_ref, out_ref):
    block = out_ref.shape[2]
    top_k, tok_mb = slots_ref.shape[1:]
    row = lax.broadcasted_iota(jnp.int32, (block, tok_mb), 0) + pl.program_id(1) * block
    hit = jnp.zeros((block, tok_mb), jnp.bool_)
    for k in range(top_k):
        hit = hit | (slots_ref[0, k:k + 1, :] == row)
    pick = jnp.where(hit, 1.0, 0.0).astype(jnp.bfloat16)
    out_ref[0, 0] = jnp.dot(pick, tok_ref[0], preferred_element_type=jnp.float32).astype(jnp.bfloat16)


def dispatch(slots_t, tokens, plane, block):
    n_src, tok_mb, hidden = tokens.shape
    top_k = slots_t.shape[1]
    return pl.pallas_call(
        dispatch_kernel,
        grid=(n_src, plane),
        in_specs=[
            pl.BlockSpec((1, top_k, tok_mb), lambda s, p: (s, 0, 0)),
            pl.BlockSpec((1, tok_mb, hidden), lambda s, p: (s, 0, 0)),
        ],
        out_specs=pl.BlockSpec((1, 1, block, hidden), lambda s, p: (p, s, 0, 0)),
        out_shape=jax.ShapeDtypeStruct((plane, n_src, block, hidden), jnp.bfloat16),
        cost_estimate=pl.CostEstimate(flops=2 * n_src * plane * block * tok_mb * hidden, bytes_accessed=n_src * plane * block * hidden * 2, transcendentals=0),
    )(slots_t, tokens)


def combine_kernel(slots_ref, gates_ref, rows_ref, out_ref):
    block = rows_ref.shape[2]
    tok_mb, top_k = slots_ref.shape[1:]
    p = pl.program_id(1)
    col = lax.broadcasted_iota(jnp.int32, (tok_mb, block), 1) + p * block
    weight = jnp.zeros((tok_mb, block), jnp.float32)
    for k in range(top_k):
        weight = weight + jnp.where(slots_ref[0, :, k:k + 1] == col, gates_ref[0, :, k:k + 1], 0.0)
    high = weight.astype(jnp.bfloat16)
    low = (weight - high.astype(jnp.float32)).astype(jnp.bfloat16)
    rows = rows_ref[0, 0]
    part = jnp.dot(high, rows, preferred_element_type=jnp.float32) + jnp.dot(low, rows, preferred_element_type=jnp.float32)

    @pl.when(p == 0)
    def _():
        out_ref[0] = part

    @pl.when(p != 0)
    def _():
        out_ref[0] += part


def combine(slots, gates, rows):
    plane, n_src, block, hidden = rows.shape
    tok_mb, top_k = slots.shape[1:]
    return pl.pallas_call(
        combine_kernel,
        grid=(n_src, plane),
        in_specs=[
            pl.BlockSpec((1, tok_mb, top_k), lambda s, p: (s, 0, 0)),
            pl.BlockSpec((1, tok_mb, top_k), lambda s, p: (s, 0, 0)),
            pl.BlockSpec((1, 1, block, hidden), lambda s, p: (p, s, 0, 0)),
        ],
        out_specs=pl.BlockSpec((1, tok_mb, hidden), lambda s, p: (s, 0, 0)),
        out_shape=jax.ShapeDtypeStruct((n_src, tok_mb, hidden), jnp.float32),
        cost_estimate=pl.CostEstimate(flops=4 * n_src * plane * block * tok_mb * hidden, bytes_accessed=n_src * plane * block * hidden * 4, transcendentals=0),
    )(slots, gates, rows)


def expert_ffn(rows, mat_up1, mat_up3, mat_down):
    gate_in = jnp.einsum("pseci,eig->psecg", rows, mat_up1, preferred_element_type=jnp.float32)
    lin_in = jnp.einsum("pseci,eig->psecg", rows, mat_up3, preferred_element_type=jnp.float32)
    hidden = (jax.nn.silu(gate_in) * lin_in).astype(jnp.bfloat16)
    return jnp.einsum("psecf,efh->psech", hidden, mat_down, preferred_element_type=jnp.float32).astype(jnp.bfloat16)


def solution(mesh):
    n_z = mesh.shape["ez"]
    plane = mesh.shape["ey"] * mesh.shape["ex"]
    n_dev = n_z * plane
    tok_spec = P(None, MESH_AXES, None)
    route_spec = P(None, None, MESH_AXES, None)
    weight_spec = P(None, MESH_AXES, None, None)

    def device_body(tokens_in, expert_ids, gate_vals, w_up1, w_up3, w_down):
        n_layers, n_micro, tok_mb, top_k = expert_ids.shape
        exp_dev = w_up1.shape[1]
        hidden_size = tokens_in.shape[-1]
        experts = exp_dev * n_dev
        capacity = capacity_of(tok_mb, top_k, experts)
        block = exp_dev * capacity
        slots = slot_table(expert_ids, experts, capacity)
        routes = jnp.concatenate([slots.astype(jnp.float32), gate_vals], axis=-1)
        routes = lax.all_gather(routes, "ez", axis=2)
        first_slot = lax.axis_index("ez") * (plane * block)
        slots = routes[..., :top_k].astype(jnp.int32) - first_slot
        gates = routes[..., top_k:]
        slots_t = jnp.swapaxes(slots, -1, -2)
        batches = [tokens_in[mb] for mb in range(n_micro)]
        for layer in range(n_layers):
            for mb in range(n_micro):
                tokens = batches[mb]
                column = lax.all_gather(tokens, "ez", axis=0)
                send = dispatch(slots_t[layer, mb], column, plane, block)
                recv = lax.all_to_all(send, PLANE_AXES, 0, 0, tiled=True)
                recv = recv.reshape(plane, n_z, exp_dev, capacity, hidden_size)
                out = expert_ffn(recv, w_up1[layer], w_up3[layer], w_down[layer])
                back = lax.all_to_all(out.reshape(plane, n_z, block, hidden_size), PLANE_AXES, 0, 0, tiled=True)
                part = combine(slots[layer, mb], gates[layer, mb], back)
                moe_sum = lax.psum_scatter(part, "ez", scatter_dimension=0, tiled=False)
                batches[mb] = (tokens.astype(jnp.float32) + ROUTE_SCALE * moe_sum).astype(jnp.bfloat16)
        return jnp.stack(batches)

    return jax.shard_map(device_body, mesh=mesh, in_specs=(tok_spec, route_spec, route_spec, weight_spec, weight_spec, weight_spec), out_specs=tok_spec, check_vma=False)
```

```python
import functools

import jax
import jax.numpy as jnp
from jax import lax
from jax.experimental import pallas as pl
from jax.experimental.pallas import tpu as pltpu
from jax.sharding import PartitionSpec as P

ROUTE_SCALE = 2.5
MESH_AXES = ("ez", "ey", "ex")
N_Z = 4
N_PEER = 4
SEND_SLOTS = 3
VMEM_LIMIT = 67043328
COLUMN = 512


def capacity_of(tok_mb, top_k, experts):
    return 2 * ((tok_mb * top_k + experts - 1) // experts)


def slot_table(ids, experts, capacity):
    chosen = (ids[..., None] == jnp.arange(experts)).astype(jnp.int32)
    per_expert = jnp.sum(chosen, axis=-2)
    token_rank = jnp.cumsum(per_expert, axis=-2) - per_expert
    slot_pos = jnp.sum(chosen * token_rank[..., None, :], axis=-1)
    return ids * capacity + slot_pos


def moe_kernel(capacity, tok_in, slots_row, slots_col, gates_col, w_up1, w_up3, w_down,
               out, d_land, r_land, c_land, x_up1, x_up3, x_down,
               col, d_buf, r_buf, part, v_up1, v_up3, v_down, stage, sum_stage, w_hi, w_lo,
               ag_send, ag_recv, d_send, d_recv, r_send, r_recv, c_send, c_recv, x_send, x_recv, load_sem, copy_sem, self_sem):
    n_layers, n_micro = slots_row.shape[:2]
    top_k, tok_mb = slots_row.shape[3:]
    hidden = col.shape[-1]
    exp_dev = w_up1.shape[1]
    block = d_buf.shape[2]
    column = min(COLUMN, hidden)
    iz, iy, ie = lax.axis_index("ez"), lax.axis_index("ey"), lax.axis_index("ex")
    ix, ic = ie // 2, ie % 2
    edge = jnp.minimum(iz, N_Z - 1 - iz)
    low = iz < N_Z // 2
    is_end = edge == 0
    is_mid = edge == 1
    mesh_id = pl.DeviceIdType.MESH

    def peer_chip(r):
        return (iy + r // 2) % 2, (ix + r % 2) % 2

    def peer(r):
        py, px = peer_chip(r)
        return (iz, py, px * 2 + ic)

    def along_z(z):
        return (z, iy, ie)

    partner = (iz, iy, ix * 2 + (1 - ic))
    inner_z = jnp.where(low, jnp.where(is_end, 1, 2), jnp.where(is_end, 2, 1))
    outer_z = jnp.where(low, 0, N_Z - 1)

    def row_of(k):
        pos = jnp.where(k == 0, 3, jnp.where(k == 1, 2, jnp.where(k == 2, 1 - edge, edge)))
        return jnp.where(low, pos, N_Z - 1 - pos)

    barrier = pltpu.get_barrier_semaphore()
    for r in range(1, N_PEER):
        pl.semaphore_signal(barrier, inc=1, device_id=peer(r), device_id_type=mesh_id)
    for t in range(1, N_Z):
        pl.semaphore_signal(barrier, inc=1, device_id=along_z((iz + t) % N_Z), device_id_type=mesh_id)
    pl.semaphore_signal(barrier, inc=1, device_id=partner, device_id_type=mesh_id)
    pl.semaphore_wait(barrier, N_PEER + N_Z - 1)

    def remote(src, dst, send_sem, recv_sem, device):
        return pltpu.make_async_remote_copy(src_ref=src, dst_ref=dst, send_sem=send_sem, recv_sem=recv_sem, device_id=device, device_id_type=mesh_id)

    def gather_copy(m, t):
        return remote(col.at[m, iz], col.at[m, iz], ag_send.at[m, t - 1], ag_recv.at[m, iz], along_z((iz + t) % N_Z))

    def gather_start(m):
        for t in (2, 1, 3):
            gather_copy(m, t).start()

    def gather_sent(m):
        for t in range(1, N_Z):
            gather_copy(m, t).wait_send()

    def gather_wait(m, s):
        remote(col.at[m, s], col.at[m, s], ag_send.at[m, 0], ag_recv.at[m, s], partner).wait_recv()

    def d_copy(m, s, slot, r):
        if r == 0:
            return pltpu.make_async_copy(d_buf.at[slot, 0], d_land.at[m, s, 0], self_sem)
        return remote(d_buf.at[slot, r], d_land.at[m, s, r], d_send.at[slot, r], d_recv.at[m, s, r], peer(r))

    def r_copy(m, s, slot, r):
        if r == 0:
            return pltpu.make_async_copy(r_buf.at[slot, 0], r_land.at[m, s, 0], self_sem)
        return remote(r_buf.at[slot, r], r_land.at[m, s, r], r_send.at[slot, r], r_recv.at[m, s, r], peer(r))

    def buffer_free(copy, m, s, count):
        @pl.when(count >= SEND_SLOTS)
        def _():
            for r in range(1, N_PEER):
                copy(m, s, count % SEND_SLOTS, r).wait_send()

    def dispatch(l, m, s, count):
        slot = count % SEND_SLOTS
        buffer_free(d_copy, m, s, count)
        tokens = col[m, s]
        picks = slots_row[l, m, s]
        for r in range(N_PEER):
            py, px = peer_chip(r)
            row = lax.broadcasted_iota(jnp.int32, (block, tok_mb), 0) + (py * 2 + px) * block
            hit = jnp.zeros((block, tok_mb), jnp.bool_)
            for k in range(top_k):
                hit = hit | (picks[k:k + 1, :] == row)
            pick = jnp.where(hit, 1.0, 0.0).astype(jnp.bfloat16)
            d_buf[slot, r] = jnp.dot(pick, tokens, preferred_element_type=jnp.float32).astype(jnp.bfloat16)
            d_copy(m, s, slot, r).start()
        d_copy(m, s, slot, 0).wait()

    def dispatch_own(l, m, count):
        dispatch(l, m, iz, count)

    def dispatch_rest(l, m, count):
        def body(k, carry):
            s = row_of(k)
            gather_wait(m, s)
            dispatch(l, m, s, count + k)
            return carry
        lax.fori_loop(0, N_Z - 1, body, 0)

    def ffn(l, m, k, count):
        s = row_of(k)
        slot = count % SEND_SLOTS
        for r in range(1, N_PEER):
            d_copy(m, s, 0, r).wait_recv()
        load = pltpu.make_async_copy(d_land.at[m, s], stage, copy_sem)
        load.start()
        buffer_free(r_copy, m, s, count)
        load.wait()

        def one_expert(j, carry):
            at = pl.multiple_of(j * capacity, 16)
            rows = stage[:, pl.ds(at, capacity), :].reshape(N_PEER * capacity, hidden)
            gate_in = jnp.dot(rows, v_up1[j], preferred_element_type=jnp.float32)
            lin_in = jnp.dot(rows, v_up3[j], preferred_element_type=jnp.float32)
            act = (jax.nn.silu(gate_in) * lin_in).astype(jnp.bfloat16)
            res = jnp.dot(act, v_down[j], preferred_element_type=jnp.float32).astype(jnp.bfloat16)
            r_buf[slot, :, pl.ds(at, capacity), :] = res.reshape(N_PEER, capacity, hidden)
            return carry
        lax.fori_loop(0, 2 * exp_dev, one_expert, 0)
        for r in range(1, N_PEER):
            r_copy(m, s, slot, r).start()
        r_copy(m, s, slot, 0).start()
        r_copy(m, s, slot, 0).wait()

    def chain_copy(m, s, kind, to_inner):
        return remote(part.at[s], c_land.at[m, kind], c_send.at[s], c_recv.at[m, kind], along_z(inner_z if to_inner else outer_z))

    def chain_arrival(m, kind):
        remote(sum_stage, c_land.at[m, kind], c_send.at[0], c_recv.at[m, kind], partner).wait_recv()
        load = pltpu.make_async_copy(c_land.at[m, kind], sum_stage, copy_sem)
        load.start()
        load.wait()

    def part_sent(m, s):
        chain_copy(m, s, 0, True).wait_send()

    def combine(l, m, k, first):
        s = row_of(k)
        for r in range(1, N_PEER):
            r_copy(m, s, 0, r).wait_recv()
        load = pltpu.make_async_copy(r_land.at[m, s], stage, copy_sem)
        load.start()
        lane = lax.broadcasted_iota(jnp.int32, (1, N_PEER * block), 1)
        target = lane
        for r in range(N_PEER):
            py, px = peer_chip(r)
            inside = (lane >= r * block) & (lane < (r + 1) * block)
            target = jnp.where(inside, lane + (py * 2 + px - r) * block, target)
        picks, gates = slots_col[l, m, s], gates_col[l, m, s]
        weight = jnp.zeros((tok_mb, N_PEER * block), jnp.float32)
        for j in range(top_k):
            weight = weight + jnp.where(picks[:, j:j + 1] == target, gates[:, j:j + 1], 0.0)
        high = weight.astype(jnp.bfloat16)
        w_hi[...] = high
        w_lo[...] = (weight - high.astype(jnp.float32)).astype(jnp.bfloat16)
        if not first:
            @pl.when(k < N_Z - 1)
            def _():
                part_sent(m, s)
        load.wait()

        def one_column(n, carry):
            cols = pl.ds(pl.multiple_of(n * column, column), column)
            rows = stage[:, :, cols].reshape(N_PEER * block, column)
            total = jnp.dot(w_hi[...], rows, preferred_element_type=jnp.float32)
            total = total + jnp.dot(w_lo[...], rows, preferred_element_type=jnp.float32)
            part[s, :, cols] = total
            return carry
        lax.fori_loop(0, hidden // column, one_column, 0)

        @pl.when(is_end & (k < N_Z - 1))
        def _():
            chain_copy(m, s, k, True).start()

    def forward(m, step):
        @pl.when(is_mid)
        def _():
            s = row_of(step)
            chain_arrival(m, (0, 1, 3)[step])
            part[s] = part[s] + sum_stage[...]
            chain_copy(m, s, (3, 4, 4)[step], step < 2).start()

    def combine_step(l, m, k, first):
        combine(l, m, k, first)
        for step in range(N_Z - 1):
            @pl.when(k == step + 1)
            def _():
                forward(m, step)

    def finish(m):
        gather_sent(m)

        @pl.when(is_mid)
        def _():
            chain_arrival(m, 2)
            part[iz] = part[iz] + sum_stage[...]
        chain_arrival(m, 4)
        total = part[iz] + sum_stage[...]
        col[m, iz] = (col[m, iz].astype(jnp.float32) + ROUTE_SCALE * total).astype(jnp.bfloat16)

    sources = (w_up1, w_up3, w_down)
    crossed = (x_up1, x_up3, x_down)
    resident = (v_up1, v_up3, v_down)

    def cross_copy(l, a):
        return remote(sources[a].at[l], crossed[a].at[l], x_send.at[l, a], x_recv.at[l, a], partner)

    def weight_loads(l):
        own = [pltpu.make_async_copy(sources[a].at[l], resident[a].at[pl.ds(ic * exp_dev, exp_dev)], load_sem.at[a, 0]) for a in range(3)]
        other = [pltpu.make_async_copy(crossed[a].at[l], resident[a].at[pl.ds((1 - ic) * exp_dev, exp_dev)], load_sem.at[a, 1]) for a in range(3)]
        return own, other

    def weights_start(l):
        own, other = weight_loads(l)
        for copy in own:
            copy.start()
        for a in range(3):
            cross_copy(l, a).wait_recv()
            other[a].start()

    def weights_wait(l):
        own, other = weight_loads(l)
        for copy in own + other:
            copy.wait()

    first_load = [pltpu.make_async_copy(tok_in.at[m], col.at[m, iz], load_sem.at[m, 0]) for m in range(n_micro)]
    for copy in first_load:
        copy.start()
    for m in range(n_micro):
        first_load[m].wait()
        gather_start(m)
    for l in range(n_layers):
        for a in range(3):
            cross_copy(l, a).start()
    dispatch_own(0, 0, 0)
    dispatch_rest(0, 0, 1)
    weights_start(0)
    for l in range(n_layers):
        base = l * 2 * N_Z
        dispatch_own(l, 1, base + N_Z)
        weights_wait(l)

        def ffn_first(k, carry):
            ffn(l, 0, k, base + k)
            return carry
        lax.fori_loop(0, N_Z, ffn_first, 0)
        dispatch_rest(l, 1, base + N_Z + 1)

        def ffn_second(k, carry):
            ffn(l, 1, k, base + N_Z + k)
            combine_step(l, 0, k, l == 0)
            return carry
        lax.fori_loop(0, N_Z, ffn_second, 0)
        last = l == n_layers - 1
        if not last:
            weights_start(l + 1)
        finish(0)
        if not last:
            gather_start(0)
            dispatch_own(l + 1, 0, base + 2 * N_Z)

        def combine_second(k, carry):
            combine_step(l, 1, k, False)
            return carry
        lax.fori_loop(0, N_Z, combine_second, 0)
        if not last:
            dispatch_rest(l + 1, 0, base + 2 * N_Z + 1)
        finish(1)
        if not last:
            gather_start(1)

    results = [pltpu.make_async_copy(col.at[m, iz], out.at[m], load_sem.at[m, 0]) for m in range(n_micro)]
    for copy in results:
        copy.start()
    for slot in range(SEND_SLOTS):
        for r in range(1, N_PEER):
            d_copy(0, 0, slot, r).wait_send()
            r_copy(0, 0, slot, r).wait_send()
    for k in range(N_Z - 1):
        part_sent(0, row_of(k))
    for l in range(n_layers):
        for a in range(3):
            cross_copy(l, a).wait_send()
    for copy in results:
        copy.wait()


def solution(mesh):
    n_dev = mesh.shape["ez"] * mesh.shape["ey"] * mesh.shape["ex"]
    tok_spec = P(None, MESH_AXES, None)
    route_spec = P(None, None, MESH_AXES, None)
    weight_spec = P(None, MESH_AXES, None, None)

    def device_body(tokens_in, expert_ids, gate_vals, w_up1, w_up3, w_down):
        n_layers, n_micro, tok_mb, top_k = expert_ids.shape
        exp_dev = w_up1.shape[1]
        hidden, ffn_dim = w_up1.shape[2:]
        experts = exp_dev * n_dev
        capacity = capacity_of(tok_mb, top_k, experts)
        block = 2 * exp_dev * capacity
        slots = slot_table(expert_ids, experts, capacity)
        routes = jnp.concatenate([slots.astype(jnp.float32), gate_vals], axis=-1)
        routes = lax.all_gather(routes, "ez", axis=2)
        slots = routes[..., :top_k].astype(jnp.int32) - lax.axis_index("ez") * (N_PEER * block)
        gates = routes[..., top_k:]
        vmem, any_space = pl.BlockSpec(memory_space=pltpu.VMEM), pl.BlockSpec(memory_space=pl.ANY)
        bf16, f32, dma = jnp.bfloat16, jnp.float32, pltpu.SemaphoreType.DMA
        rows_shape = jax.ShapeDtypeStruct((n_micro, N_Z, N_PEER, block, hidden), bf16)
        outs = pl.pallas_call(
            functools.partial(moe_kernel, capacity),
            in_specs=[any_space, vmem, vmem, vmem, any_space, any_space, any_space],
            out_specs=[any_space] * 7,
            out_shape=[
                jax.ShapeDtypeStruct(tokens_in.shape, bf16),
                rows_shape,
                rows_shape,
                jax.ShapeDtypeStruct((n_micro, 5, tok_mb, hidden), f32),
                jax.ShapeDtypeStruct(w_up1.shape, bf16),
                jax.ShapeDtypeStruct(w_up3.shape, bf16),
                jax.ShapeDtypeStruct(w_down.shape, bf16),
            ],
            scratch_shapes=[
                pltpu.VMEM((n_micro, N_Z, tok_mb, hidden), bf16),
                pltpu.VMEM((SEND_SLOTS, N_PEER, block, hidden), bf16),
                pltpu.VMEM((SEND_SLOTS, N_PEER, block, hidden), bf16),
                pltpu.VMEM((N_Z, tok_mb, hidden), f32),
                pltpu.VMEM((2 * exp_dev, hidden, ffn_dim), bf16),
                pltpu.VMEM((2 * exp_dev, hidden, ffn_dim), bf16),
                pltpu.VMEM((2 * exp_dev, ffn_dim, hidden), bf16),
                pltpu.VMEM((N_PEER, block, hidden), bf16),
                pltpu.VMEM((tok_mb, hidden), f32),
                pltpu.VMEM((tok_mb, N_PEER * block), bf16),
                pltpu.VMEM((tok_mb, N_PEER * block), bf16),
                dma((n_micro, N_Z - 1)),
                dma((n_micro, N_Z)),
                dma((SEND_SLOTS, N_PEER)),
                dma((n_micro, N_Z, N_PEER)),
                dma((SEND_SLOTS, N_PEER)),
                dma((n_micro, N_Z, N_PEER)),
                dma((N_Z,)),
                dma((n_micro, 5)),
                dma((n_layers, 3)),
                dma((n_layers, 3)),
                dma((3, 2)),
                dma(()),
                dma(()),
            ],
            compiler_params=pltpu.CompilerParams(collective_id=0, has_side_effects=True, vmem_limit_bytes=VMEM_LIMIT),
            name="moe_layers",
        )(tokens_in, jnp.swapaxes(slots, -1, -2), slots, gates, w_up1, w_up3, w_down)
        return outs[0]

    return jax.shard_map(device_body, mesh=mesh, in_specs=(tok_spec, route_spec, route_spec, weight_spec, weight_spec, weight_spec), out_specs=tok_spec, check_vma=False)
```

```python
import functools

import jax
import jax.numpy as jnp
from jax import lax
from jax.experimental import pallas as pl
from jax.experimental.pallas import tpu as pltpu
from jax.sharding import PartitionSpec as P

ROUTE_SCALE = 2.5
MESH_AXES = ("ez", "ey", "ex")
N_Z = 4
N_PEER = 4
D_SLOTS = 6
R_SLOTS = 3
VMEM_LIMIT = 67043328
COLUMN = 512


def capacity_of(tok_mb, top_k, experts):
    return 2 * ((tok_mb * top_k + experts - 1) // experts)


def slot_table(ids, experts, capacity):
    chosen = (ids[..., None] == jnp.arange(experts)).astype(jnp.int32)
    per_expert = jnp.sum(chosen, axis=-2)
    token_rank = jnp.cumsum(per_expert, axis=-2) - per_expert
    slot_pos = jnp.sum(chosen * token_rank[..., None, :], axis=-1)
    return ids * capacity + slot_pos


def moe_kernel(capacity, top_k, tok_in, routes_in, w_up1, w_up3, w_down,
               out, d_land, r_land, c_land, x_up1, x_up3, x_down,
               col, d_buf, r_buf, part, v_up1, v_up3, v_down, stage, sum_stage, w_hi, w_lo, routes, routes_near,
               swap_send, ag_send, ag_recv, d_send, d_recv, r_send, r_recv, c_send, c_recv, x_send, x_recv,
               t_send, t_recv, n_send, n_recv, load_sem, copy_sem, self_sem):
    n_micro, n_layers = routes_in.shape[:2]
    tok_mb = routes_in.shape[3]
    hidden = col.shape[-1]
    exp_dev = w_up1.shape[1]
    block = d_buf.shape[2]
    column = min(COLUMN, hidden)
    iz, iy, ie = lax.axis_index("ez"), lax.axis_index("ey"), lax.axis_index("ex")
    ix, ic = ie // 2, ie % 2
    edge = jnp.minimum(iz, N_Z - 1 - iz)
    low = iz < N_Z // 2
    is_end = edge == 0
    is_mid = edge == 1
    mesh_id = pl.DeviceIdType.MESH

    def peer_chip(r):
        return (iy + r // 2) % 2, (ix + r % 2) % 2

    def peer(r, z=None):
        py, px = peer_chip(r)
        return (iz if z is None else z, py, px * 2 + ic)

    def near_axis(s):
        return 1 + s % 2

    def far_axis(s):
        return 2 - s % 2

    def relation(s, i):
        return (0, near_axis(s), far_axis(s), 3)[i]

    partner = (iz, iy, ix * 2 + (1 - ic))
    inner_z = jnp.where(low, jnp.where(is_end, 1, 2), jnp.where(is_end, 2, 1))
    outer_z = jnp.where(low, 0, N_Z - 1)

    def row_of(k):
        pos = jnp.where(k == 0, 3, jnp.where(k == 1, 2, jnp.where(k == 2, 1 - edge, edge)))
        return jnp.where(low, pos, N_Z - 1 - pos)

    def near_row(j):
        pos = jnp.where(j == 0, 1 - edge, j + 1)
        return jnp.where(low, pos, N_Z - 1 - pos)

    barrier = pltpu.get_barrier_semaphore()
    for r in range(1, N_PEER):
        pl.semaphore_signal(barrier, inc=1, device_id=peer(r), device_id_type=mesh_id)
    for t in range(1, N_Z):
        z = (iz + t) % N_Z
        pl.semaphore_signal(barrier, inc=1, device_id=peer(0, z), device_id_type=mesh_id)
        pl.semaphore_signal(barrier, inc=1, device_id=peer(near_axis(z), z), device_id_type=mesh_id)
    pl.semaphore_signal(barrier, inc=1, device_id=partner, device_id_type=mesh_id)
    pl.semaphore_wait(barrier, N_PEER + 2 * (N_Z - 1))

    def remote(src, dst, send_sem, recv_sem, device):
        return pltpu.make_async_remote_copy(src_ref=src, dst_ref=dst, send_sem=send_sem, recv_sem=recv_sem, device_id=device, device_id_type=mesh_id)

    def table_copy(t):
        return remote(routes_in, routes.at[iz], t_send.at[t - 1], t_recv.at[iz], peer(0, (iz + t) % N_Z))

    def near_table_copy(t):
        return remote(routes_in, routes_near.at[iz], n_send.at[t], n_recv.at[iz], peer(near_axis(iz), (iz + t) % N_Z))

    def tables_wait():
        for t in range(1, N_Z):
            z = (iz + t) % N_Z
            remote(routes_in, routes.at[z], t_send.at[0], t_recv.at[z], partner).wait_recv()
        for z in range(N_Z):
            remote(routes_in, routes_near.at[z], n_send.at[0], n_recv.at[z], partner).wait_recv()

    def swap_copy(m):
        return remote(col.at[m, 0, iz], col.at[m, 1, iz], swap_send.at[m], ag_recv.at[m, 1, iz], peer(near_axis(iz)))

    def gather_copy(m, t, s, to_inner, sem):
        return remote(col.at[m, t, s], col.at[m, t, s], ag_send.at[m, t, sem], ag_recv.at[m, t, s], peer(0, inner_z if to_inner else outer_z))

    def gather_wait(m, t, s):
        remote(col.at[m, t, s], col.at[m, t, s], ag_send.at[m, t, 0], ag_recv.at[m, t, s], partner).wait_recv()

    def gather_start(m, t):
        @pl.when(is_mid)
        def _():
            gather_copy(m, t, iz, False, 1).start()
        gather_copy(m, t, iz, True, 0).start()

    def pump(m, j):
        s = near_row(j)
        for t in range(2):
            gather_wait(m, t, s)

            @pl.when(is_mid)
            def _():
                gather_copy(m, t, s, j == 0, 2 + j).start()

    def gather_sent(m):
        swap_copy(m).wait_send()
        for t in range(2):
            gather_copy(m, t, iz, True, 0).wait_send()

            @pl.when(is_mid)
            def _():
                for sem in range(1, 2 + N_Z - 1):
                    gather_copy(m, t, iz, False, sem).wait_send()

    def d_self(m, t, s, slot):
        return pltpu.make_async_copy(d_buf.at[slot, 0], d_land.at[m, s, t], self_sem)

    def d_copy(m, t, s, slot):
        return remote(d_buf.at[slot, 1], d_land.at[m, s, 2 + t], d_send.at[slot], d_recv.at[m, s, t], peer(far_axis(s)))

    def r_copy(m, s, slot, i):
        if i == 0:
            return pltpu.make_async_copy(r_buf.at[slot, 0], r_land.at[m, s, 0], self_sem)
        return remote(r_buf.at[slot, i], r_land.at[m, s, i], r_send.at[slot, i], r_recv.at[m, s, i], peer(relation(s, i)))

    def dispatch(l, m, t, s, count):
        slot = count % D_SLOTS

        @pl.when(count >= D_SLOTS)
        def _():
            d_copy(m, t, s, slot).wait_send()
        tokens = col[m, t, s]
        picks = (routes_near if t else routes)[s, m, l]
        row = lax.broadcasted_iota(jnp.int32, (block, tok_mb), 0)
        for dest in (1, 0):
            py, px = peer_chip(far_axis(s) if dest else 0)
            first = iz * (N_PEER * block) + (py * 2 + px) * block
            wanted = (row + first).astype(jnp.float32)
            hit = jnp.zeros((block, tok_mb), jnp.bool_)
            for k in range(top_k):
                hit = hit | (picks[k:k + 1, :] == wanted)
            pick = jnp.where(hit, 1.0, 0.0).astype(jnp.bfloat16)
            d_buf[slot, dest] = jnp.dot(pick, tokens, preferred_element_type=jnp.float32).astype(jnp.bfloat16)
            if dest:
                d_copy(m, t, s, slot).start()
        d_self(m, t, s, slot).start()
        d_self(m, t, s, slot).wait()

    def dispatch_near(l, m, count):
        gather_wait(m, 1, iz)
        gather_start(m, 1)
        dispatch(l, m, 1, iz, count)

    def dispatch_row(l, m, j, count):
        for t in range(2):
            dispatch(l, m, t, near_row(j), count + t)

    def dispatch_rest(l, m, count):
        def body(j, carry):
            dispatch_row(l, m, j, count + 2 * j)
            return carry
        lax.fori_loop(0, N_Z - 1, body, 0)

    def ffn(l, m, k, count):
        s = row_of(k)
        slot = count % R_SLOTS
        for t in range(2):
            d_copy(m, t, s, 0).wait_recv()
        load = pltpu.make_async_copy(d_land.at[m, s], stage, copy_sem)
        load.start()

        @pl.when(count >= R_SLOTS)
        def _():
            for i in range(1, N_PEER):
                r_copy(m, s, slot, i).wait_send()
        load.wait()

        def one_expert(j, carry):
            at = pl.multiple_of(j * capacity, 16)
            rows = stage[:, pl.ds(at, capacity), :].reshape(N_PEER * capacity, hidden)
            gate_in = jnp.dot(rows, v_up1[j], preferred_element_type=jnp.float32)
            lin_in = jnp.dot(rows, v_up3[j], preferred_element_type=jnp.float32)
            act = (jax.nn.silu(gate_in) * lin_in).astype(jnp.bfloat16)
            res = jnp.dot(act, v_down[j], preferred_element_type=jnp.float32).astype(jnp.bfloat16)
            r_buf[slot, :, pl.ds(at, capacity), :] = res.reshape(N_PEER, capacity, hidden)
            return carry
        lax.fori_loop(0, 2 * exp_dev, one_expert, 0)
        for i in (3, 1, 2, 0):
            r_copy(m, s, slot, i).start()
        r_copy(m, s, slot, 0).wait()

    def chain_copy(m, s, kind, to_inner):
        return remote(part.at[s], c_land.at[m, kind], c_send.at[s], c_recv.at[m, kind], peer(0, inner_z if to_inner else outer_z))

    def chain_arrival(m, kind):
        remote(sum_stage, c_land.at[m, kind], c_send.at[0], c_recv.at[m, kind], partner).wait_recv()
        load = pltpu.make_async_copy(c_land.at[m, kind], sum_stage, copy_sem)
        load.start()
        load.wait()

    def part_sent(m, s):
        chain_copy(m, s, 0, True).wait_send()

    def combine(l, m, k, first):
        s = row_of(k)
        for i in range(1, N_PEER):
            r_copy(m, s, 0, i).wait_recv()
        load = pltpu.make_async_copy(r_land.at[m, s], stage, copy_sem)
        load.start()
        line = lax.broadcasted_iota(jnp.int32, (N_PEER * block, tok_mb), 0)
        target = line
        for i in range(N_PEER):
            py, px = peer_chip(relation(s, i))
            inside = (line >= i * block) & (line < (i + 1) * block)
            target = jnp.where(inside, line + (iz * (N_PEER * block) + (py * 2 + px - i) * block), target)
        target = target.astype(jnp.float32)
        table = routes[s, m, l]
        weight = jnp.zeros((N_PEER * block, tok_mb), jnp.float32)
        for j in range(top_k):
            weight = weight + jnp.where(table[j:j + 1, :] == target, table[8 + j:9 + j, :], 0.0)
        weight = weight.T
        high = weight.astype(jnp.bfloat16)
        w_hi[...] = high
        w_lo[...] = (weight - high.astype(jnp.float32)).astype(jnp.bfloat16)
        if not first:
            @pl.when(k < N_Z - 1)
            def _():
                part_sent(m, s)
        load.wait()

        def one_column(n, carry):
            cols = pl.ds(pl.multiple_of(n * column, column), column)
            rows = stage[:, :, cols].reshape(N_PEER * block, column)
            total = jnp.dot(w_hi[...], rows, preferred_element_type=jnp.float32)
            total = total + jnp.dot(w_lo[...], rows, preferred_element_type=jnp.float32)
            part[s, :, cols] = total
            return carry
        lax.fori_loop(0, hidden // column, one_column, 0)

        @pl.when(is_end & (k < N_Z - 1))
        def _():
            chain_copy(m, s, k, True).start()

    def forward(m, step):
        @pl.when(is_mid)
        def _():
            s = row_of(step)
            chain_arrival(m, (0, 1, 3)[step])
            part[s] = part[s] + sum_stage[...]
            chain_copy(m, s, (3, 4, 4)[step], step < 2).start()

    def combine_step(l, m, k, first):
        combine(l, m, k, first)
        for step in range(N_Z - 1):
            @pl.when(k == step + 1)
            def _():
                forward(m, step)

    def intake_step(l, m, k, count):
        @pl.when(k == 0)
        def _():
            dispatch_near(l, m, count)
        for j in range(N_Z - 1):
            @pl.when(k == j + 1)
            def _():
                pump(m, j)

    def finish(m):
        @pl.when(is_mid)
        def _():
            chain_arrival(m, 2)
            part[iz] = part[iz] + sum_stage[...]
        chain_arrival(m, 4)
        total = part[iz] + sum_stage[...]
        col[m, 0, iz] = (col[m, 0, iz].astype(jnp.float32) + ROUTE_SCALE * total).astype(jnp.bfloat16)

    def share(m):
        swap_copy(m).start()
        gather_start(m, 0)

    sources = (w_up1, w_up3, w_down)
    crossed = (x_up1, x_up3, x_down)
    resident = (v_up1, v_up3, v_down)

    def cross_copy(l, a):
        return remote(sources[a].at[l], crossed[a].at[l], x_send.at[l, a], x_recv.at[l, a], partner)

    def weight_loads(l):
        own = [pltpu.make_async_copy(sources[a].at[l], resident[a].at[pl.ds(ic * exp_dev, exp_dev)], load_sem.at[a, 0]) for a in range(3)]
        other = [pltpu.make_async_copy(crossed[a].at[l], resident[a].at[pl.ds((1 - ic) * exp_dev, exp_dev)], load_sem.at[a, 1]) for a in range(3)]
        return own, other

    def weights_start(l):
        own, other = weight_loads(l)
        for copy in own:
            copy.start()
        for a in range(3):
            cross_copy(l, a).wait_recv()
            other[a].start()

    def weights_wait(l):
        own, other = weight_loads(l)
        for copy in own + other:
            copy.wait()

    first_load = [pltpu.make_async_copy(tok_in.at[m], col.at[m, 0, iz], load_sem.at[m, 0]) for m in range(n_micro)]
    for copy in first_load:
        copy.start()
    for t in range(1, N_Z):
        table_copy(t).start()
    for t in range(N_Z):
        near_table_copy(t).start()
    for m in range(n_micro):
        first_load[m].wait()
        swap_copy(m).start()
        if m == 0:
            gather_start(0, 0)
    for l in range(n_layers):
        for a in range(3):
            cross_copy(l, a).start()
    routes[iz] = routes_in[...]
    tables_wait()
    dispatch(0, 0, 0, iz, 0)
    dispatch_near(0, 0, 1)
    gather_start(1, 0)
    for j in range(N_Z - 1):
        pump(0, j)
        dispatch_row(0, 0, j, 2 + 2 * j)
    weights_start(0)
    for l in range(n_layers):
        last = l == n_layers - 1
        d_base, r_base = l * 4 * N_Z, l * 2 * N_Z
        d_other, d_next = d_base + 2 * N_Z, d_base + 4 * N_Z
        dispatch(l, 1, 0, iz, d_other)
        weights_wait(l)
        gather_sent(0)

        def ffn_first(k, carry):
            ffn(l, 0, k, r_base + k)
            intake_step(l, 1, k, d_other + 1)
            return carry
        lax.fori_loop(0, N_Z, ffn_first, 0)
        dispatch_rest(l, 1, d_other + 2)
        gather_sent(1)

        def ffn_second(k, carry):
            ffn(l, 1, k, r_base + N_Z + k)
            combine_step(l, 0, k, l == 0)
            return carry
        lax.fori_loop(0, N_Z, ffn_second, 0)
        if not last:
            weights_start(l + 1)
        finish(0)
        if not last:
            share(0)
            dispatch(l + 1, 0, 0, iz, d_next)

        def combine_second(k, carry):
            combine_step(l, 1, k, False)
            if not last:
                intake_step(l + 1, 0, k, d_next + 1)
            return carry
        lax.fori_loop(0, N_Z, combine_second, 0)
        if not last:
            dispatch_rest(l + 1, 0, d_next + 2)
        finish(1)
        if not last:
            share(1)

    results = [pltpu.make_async_copy(col.at[m, 0, iz], out.at[m], load_sem.at[m, 0]) for m in range(n_micro)]
    for copy in results:
        copy.start()
    for slot in range(D_SLOTS):
        d_copy(0, 0, iz, slot).wait_send()
    for slot in range(R_SLOTS):
        for i in range(1, N_PEER):
            r_copy(0, iz, slot, i).wait_send()
    for k in range(N_Z - 1):
        part_sent(0, row_of(k))
    for l in range(n_layers):
        for a in range(3):
            cross_copy(l, a).wait_send()
    for t in range(1, N_Z):
        table_copy(t).wait_send()
    for t in range(N_Z):
        near_table_copy(t).wait_send()
    for copy in results:
        copy.wait()


def solution(mesh):
    n_dev = mesh.shape["ez"] * mesh.shape["ey"] * mesh.shape["ex"]
    tok_spec = P(None, MESH_AXES, None)
    route_spec = P(None, None, MESH_AXES, None)
    weight_spec = P(None, MESH_AXES, None, None)

    def device_body(tokens_in, expert_ids, gate_vals, w_up1, w_up3, w_down):
        n_layers, n_micro, tok_mb, top_k = expert_ids.shape
        exp_dev = w_up1.shape[1]
        hidden, ffn_dim = w_up1.shape[2:]
        experts = exp_dev * n_dev
        capacity = capacity_of(tok_mb, top_k, experts)
        block = 2 * exp_dev * capacity
        slots = slot_table(expert_ids, experts, capacity)
        pad = ((0, 0), (0, 0), (0, 0), (0, 8 - top_k))
        routes = jnp.concatenate([jnp.pad(slots.astype(jnp.float32), pad), jnp.pad(gate_vals, pad)], axis=-1)
        routes = jnp.transpose(routes, (1, 0, 3, 2))
        vmem, any_space = pl.BlockSpec(memory_space=pltpu.VMEM), pl.BlockSpec(memory_space=pl.ANY)
        bf16, f32, dma = jnp.bfloat16, jnp.float32, pltpu.SemaphoreType.DMA
        rows_shape = jax.ShapeDtypeStruct((n_micro, N_Z, N_PEER, block, hidden), bf16)
        outs = pl.pallas_call(
            functools.partial(moe_kernel, capacity, top_k),
            in_specs=[any_space, vmem, any_space, any_space, any_space],
            out_specs=[any_space] * 7,
            out_shape=[
                jax.ShapeDtypeStruct(tokens_in.shape, bf16),
                rows_shape,
                rows_shape,
                jax.ShapeDtypeStruct((n_micro, 5, tok_mb, hidden), f32),
                jax.ShapeDtypeStruct(w_up1.shape, bf16),
                jax.ShapeDtypeStruct(w_up3.shape, bf16),
                jax.ShapeDtypeStruct(w_down.shape, bf16),
            ],
            scratch_shapes=[
                pltpu.VMEM((n_micro, 2, N_Z, tok_mb, hidden), bf16),
                pltpu.VMEM((D_SLOTS, 2, block, hidden), bf16),
                pltpu.VMEM((R_SLOTS, N_PEER, block, hidden), bf16),
                pltpu.VMEM((N_Z, tok_mb, hidden), f32),
                pltpu.VMEM((2 * exp_dev, hidden, ffn_dim), bf16),
                pltpu.VMEM((2 * exp_dev, hidden, ffn_dim), bf16),
                pltpu.VMEM((2 * exp_dev, ffn_dim, hidden), bf16),
                pltpu.VMEM((N_PEER, block, hidden), bf16),
                pltpu.VMEM((tok_mb, hidden), f32),
                pltpu.VMEM((tok_mb, N_PEER * block), bf16),
                pltpu.VMEM((tok_mb, N_PEER * block), bf16),
                pltpu.VMEM((N_Z,) + routes.shape, f32),
                pltpu.VMEM((N_Z,) + routes.shape, f32),
                dma((n_micro,)),
                dma((n_micro, 2, N_Z + 1)),
                dma((n_micro, 2, N_Z)),
                dma((D_SLOTS,)),
                dma((n_micro, N_Z, 2)),
                dma((R_SLOTS, N_PEER)),
                dma((n_micro, N_Z, N_PEER)),
                dma((N_Z,)),
                dma((n_micro, 5)),
                dma((n_layers, 3)),
                dma((n_layers, 3)),
                dma((N_Z - 1,)),
                dma((N_Z,)),
                dma((N_Z,)),
                dma((N_Z,)),
                dma((3, 2)),
                dma(()),
                dma(()),
            ],
            compiler_params=pltpu.CompilerParams(collective_id=0, has_side_effects=True, vmem_limit_bytes=VMEM_LIMIT),
            name="moe_layers",
        )(tokens_in, routes, w_up1, w_up3, w_down)
        return outs[0]

    return jax.shard_map(device_body, mesh=mesh, in_specs=(tok_spec, route_spec, route_spec, weight_spec, weight_spec, weight_spec), out_specs=tok_spec, check_vma=False)
```

```python
import functools

import jax
import jax.numpy as jnp
from jax import lax
from jax.experimental import pallas as pl
from jax.experimental.pallas import tpu as pltpu
from jax.sharding import PartitionSpec as P

ROUTE_SCALE = 2.5
MESH_AXES = ("ez", "ey", "ex")
N_Z = 4
N_PEER = 4
SEND_SLOTS = 4
VMEM_LIMIT = 67043328
COLUMN = 512


def capacity_of(tok_mb, top_k, experts):
    return 2 * ((tok_mb * top_k + experts - 1) // experts)


def slot_table(ids, experts, capacity):
    chosen = (ids[..., None] == jnp.arange(experts)).astype(jnp.int32)
    per_expert = jnp.sum(chosen, axis=-2)
    token_rank = jnp.cumsum(per_expert, axis=-2) - per_expert
    slot_pos = jnp.sum(chosen * token_rank[..., None, :], axis=-1)
    return ids * capacity + slot_pos


def moe_kernel(capacity, top_k, tok_in, routes_in, w_up1, w_up3, w_down,
               out, d_land, r_land, c_land, x_up1, x_up3, x_down,
               col, d_buf, r_buf, part, v_up1, v_up3, v_down, stage, sum_stage, w_hi, w_lo, routes,
               ag_send, ag_recv, d_send, d_recv, r_send, r_recv, c_send, c_recv, x_send, x_recv,
               t_send, t_recv, load_sem, copy_sem, self_sem):
    n_micro, n_layers = routes_in.shape[:2]
    tok_mb = routes_in.shape[3]
    hidden = col.shape[-1]
    exp_dev = w_up1.shape[1]
    block = d_buf.shape[2]
    column = min(COLUMN, hidden)
    iz, iy, ie = lax.axis_index("ez"), lax.axis_index("ey"), lax.axis_index("ex")
    ix, ic = ie // 2, ie % 2
    edge = jnp.minimum(iz, N_Z - 1 - iz)
    low = iz < N_Z // 2
    is_end = edge == 0
    is_mid = edge == 1
    mesh_id = pl.DeviceIdType.MESH

    def peer_chip(r):
        return (iy + r // 2) % 2, (ix + r % 2) % 2

    def peer(r, z=None):
        py, px = peer_chip(r)
        return (iz if z is None else z, py, px * 2 + ic)

    partner = (iz, iy, ix * 2 + (1 - ic))
    inner_z = jnp.where(low, jnp.where(is_end, 1, 2), jnp.where(is_end, 2, 1))
    outer_z = jnp.where(low, 0, N_Z - 1)

    def row_of(k):
        pos = jnp.where(k == 0, 3, jnp.where(k == 1, 2, jnp.where(k == 2, 1 - edge, edge)))
        return jnp.where(low, pos, N_Z - 1 - pos)

    def near_row(j):
        pos = jnp.where(j == 0, 1 - edge, j + 1)
        return jnp.where(low, pos, N_Z - 1 - pos)

    barrier = pltpu.get_barrier_semaphore()
    for r in range(1, N_PEER):
        pl.semaphore_signal(barrier, inc=1, device_id=peer(r), device_id_type=mesh_id)
    for t in range(1, N_Z):
        z = (iz + t) % N_Z
        pl.semaphore_signal(barrier, inc=1, device_id=peer(0, z), device_id_type=mesh_id)
    pl.semaphore_signal(barrier, inc=1, device_id=partner, device_id_type=mesh_id)
    pl.semaphore_wait(barrier, N_PEER + N_Z - 1)

    def remote(src, dst, send_sem, recv_sem, device):
        return pltpu.make_async_remote_copy(src_ref=src, dst_ref=dst, send_sem=send_sem, recv_sem=recv_sem, device_id=device, device_id_type=mesh_id)

    def table_copy(t):
        return remote(routes_in, routes.at[iz], t_send.at[t - 1], t_recv.at[iz], peer(0, (iz + t) % N_Z))

    def tables_wait():
        for t in range(1, N_Z):
            z = (iz + t) % N_Z
            remote(routes_in, routes.at[z], t_send.at[0], t_recv.at[z], partner).wait_recv()

    def gather_copy(m, t):
        return remote(col.at[m, iz], col.at[m, iz], ag_send.at[m, t - 1], ag_recv.at[m, iz], peer(0, (iz + t) % N_Z))

    def gather_start(m):
        for t in (2, 1, 3):
            gather_copy(m, t).start()

    def gather_sent(m):
        for t in range(1, N_Z):
            gather_copy(m, t).wait_send()

    def gather_wait(m, s):
        remote(col.at[m, s], col.at[m, s], ag_send.at[m, 0], ag_recv.at[m, s], partner).wait_recv()

    def d_copy(m, s, slot, r):
        if r == 0:
            return pltpu.make_async_copy(d_buf.at[slot, 0], d_land.at[m, s, 0], self_sem)
        return remote(d_buf.at[slot, r], d_land.at[m, s, r], d_send.at[slot, r], d_recv.at[m, s, r], peer(r))

    def r_copy(m, s, slot, r):
        if r == 0:
            return pltpu.make_async_copy(r_buf.at[slot, 0], r_land.at[m, s, 0], self_sem)
        return remote(r_buf.at[slot, r], r_land.at[m, s, r], r_send.at[slot, r], r_recv.at[m, s, r], peer(r))

    def buffer_free(copy, m, s, count):
        @pl.when(count >= SEND_SLOTS)
        def _():
            for r in range(1, N_PEER):
                copy(m, s, count % SEND_SLOTS, r).wait_send()

    def dispatch(l, m, s, count):
        slot = count % SEND_SLOTS
        buffer_free(d_copy, m, s, count)
        tokens = col[m, s]
        picks = routes[s, m, l]
        row = lax.broadcasted_iota(jnp.int32, (block, tok_mb), 0)
        for r in (3, 1, 2, 0):
            py, px = peer_chip(r)
            wanted = (row + (iz * (N_PEER * block) + (py * 2 + px) * block)).astype(jnp.float32)
            hit = jnp.zeros((block, tok_mb), jnp.bool_)
            for k in range(top_k):
                hit = hit | (picks[k:k + 1, :] == wanted)
            pick = jnp.where(hit, 1.0, 0.0).astype(jnp.bfloat16)
            d_buf[slot, r] = jnp.dot(pick, tokens, preferred_element_type=jnp.float32).astype(jnp.bfloat16)
            d_copy(m, s, slot, r).start()
        d_copy(m, s, slot, 0).wait()

    def dispatch_row(l, m, j, count):
        s = near_row(j)
        gather_wait(m, s)
        dispatch(l, m, s, count + 1 + j)

    def ffn(l, m, k, count):
        s = row_of(k)
        slot = count % SEND_SLOTS
        for r in range(1, N_PEER):
            d_copy(m, s, 0, r).wait_recv()
        load = pltpu.make_async_copy(d_land.at[m, s], stage, copy_sem)
        load.start()
        buffer_free(r_copy, m, s, count)
        load.wait()

        def one_expert(j, carry):
            at = pl.multiple_of(j * capacity, 16)
            rows = stage[:, pl.ds(at, capacity), :].reshape(N_PEER * capacity, hidden)
            gate_in = jnp.dot(rows, v_up1[j], preferred_element_type=jnp.float32)
            lin_in = jnp.dot(rows, v_up3[j], preferred_element_type=jnp.float32)
            act = (jax.nn.silu(gate_in) * lin_in).astype(jnp.bfloat16)
            res = jnp.dot(act, v_down[j], preferred_element_type=jnp.float32).astype(jnp.bfloat16)
            r_buf[slot, :, pl.ds(at, capacity), :] = res.reshape(N_PEER, capacity, hidden)
            return carry
        lax.fori_loop(0, 2 * exp_dev, one_expert, 0)
        for r in (3, 1, 2, 0):
            r_copy(m, s, slot, r).start()
        r_copy(m, s, slot, 0).wait()

    def chain_copy(m, s, kind, to_inner):
        return remote(part.at[s], c_land.at[m, kind], c_send.at[s], c_recv.at[m, kind], peer(0, inner_z if to_inner else outer_z))

    def chain_arrival(m, kind):
        remote(sum_stage, c_land.at[m, kind], c_send.at[0], c_recv.at[m, kind], partner).wait_recv()
        load = pltpu.make_async_copy(c_land.at[m, kind], sum_stage, copy_sem)
        load.start()
        load.wait()

    def part_sent(m, s):
        chain_copy(m, s, 0, True).wait_send()

    def combine(l, m, k, first):
        s = row_of(k)
        for i in range(1, N_PEER):
            r_copy(m, s, 0, i).wait_recv()
        load = pltpu.make_async_copy(r_land.at[m, s], stage, copy_sem)
        load.start()
        line = lax.broadcasted_iota(jnp.int32, (N_PEER * block, tok_mb), 0)
        target = line
        for i in range(N_PEER):
            py, px = peer_chip(i)
            inside = (line >= i * block) & (line < (i + 1) * block)
            target = jnp.where(inside, line + (iz * (N_PEER * block) + (py * 2 + px - i) * block), target)
        target = target.astype(jnp.float32)
        table = routes[s, m, l]
        weight = jnp.zeros((N_PEER * block, tok_mb), jnp.float32)
        for j in range(top_k):
            weight = weight + jnp.where(table[j:j + 1, :] == target, table[8 + j:9 + j, :], 0.0)
        weight = weight.T
        high = weight.astype(jnp.bfloat16)
        w_hi[...] = high
        w_lo[...] = (weight - high.astype(jnp.float32)).astype(jnp.bfloat16)
        if not first:
            @pl.when(k < N_Z - 1)
            def _():
                part_sent(m, s)
        load.wait()

        def one_column(n, carry):
            cols = pl.ds(pl.multiple_of(n * column, column), column)
            rows = stage[:, :, cols].reshape(N_PEER * block, column)
            total = jnp.dot(w_hi[...], rows, preferred_element_type=jnp.float32)
            total = total + jnp.dot(w_lo[...], rows, preferred_element_type=jnp.float32)
            part[s, :, cols] = total
            return carry
        lax.fori_loop(0, hidden // column, one_column, 0)

        @pl.when(is_end & (k < N_Z - 1))
        def _():
            chain_copy(m, s, k, True).start()

    def forward(m, step):
        @pl.when(is_mid)
        def _():
            s = row_of(step)
            chain_arrival(m, (0, 1, 3)[step])
            part[s] = part[s] + sum_stage[...]
            chain_copy(m, s, (3, 4, 4)[step], step < 2).start()

    def combine_step(l, m, k, first):
        combine(l, m, k, first)
        for step in range(N_Z - 1):
            @pl.when(k == step + 1)
            def _():
                forward(m, step)

    def finish(m):
        gather_sent(m)

        @pl.when(is_mid)
        def _():
            chain_arrival(m, 2)
            part[iz] = part[iz] + sum_stage[...]
        chain_arrival(m, 4)
        total = part[iz] + sum_stage[...]
        col[m, iz] = (col[m, iz].astype(jnp.float32) + ROUTE_SCALE * total).astype(jnp.bfloat16)

    sources = (w_up1, w_up3, w_down)
    crossed = (x_up1, x_up3, x_down)
    resident = (v_up1, v_up3, v_down)

    def cross_copy(l, a):
        return remote(sources[a].at[l], crossed[a].at[l], x_send.at[l, a], x_recv.at[l, a], partner)

    def weight_loads(l):
        own = [pltpu.make_async_copy(sources[a].at[l], resident[a].at[pl.ds(ic * exp_dev, exp_dev)], load_sem.at[a, 0]) for a in range(3)]
        other = [pltpu.make_async_copy(crossed[a].at[l], resident[a].at[pl.ds((1 - ic) * exp_dev, exp_dev)], load_sem.at[a, 1]) for a in range(3)]
        return own, other

    def weights_start(l):
        own, other = weight_loads(l)
        for copy in own:
            copy.start()
        for a in range(3):
            cross_copy(l, a).wait_recv()
            other[a].start()

    def weights_wait(l):
        own, other = weight_loads(l)
        for copy in own + other:
            copy.wait()

    first_load = [pltpu.make_async_copy(tok_in.at[m], col.at[m, iz], load_sem.at[m, 0]) for m in range(n_micro)]
    for copy in first_load:
        copy.start()
    for t in range(1, N_Z):
        table_copy(t).start()
    first_load[0].wait()
    gather_start(0)
    for l in range(n_layers):
        for a in range(3):
            cross_copy(l, a).start()
    routes[iz] = routes_in[...]
    first_load[1].wait()
    tables_wait()
    dispatch(0, 0, iz, 0)
    gather_start(1)

    def first_rows(j, carry):
        dispatch_row(0, 0, j, 0)
        return carry
    lax.fori_loop(0, N_Z - 1, first_rows, 0)
    weights_start(0)
    weights_wait(0)

    def first_ffn(k, carry):
        ffn(0, 0, k, k)
        return carry
    lax.fori_loop(0, N_Z, first_ffn, 0)
    turns = [(l, m) for l in range(n_layers) for m in range(n_micro)]
    for turn in range(1, len(turns)):
        (l, m), (l_prev, m_prev) = turns[turn], turns[turn - 1]
        base = turn * N_Z
        if m == 0:
            weights_start(l)
        dispatch(l, m, iz, base)

        def sums_and_rows(k, carry):
            combine_step(l_prev, m_prev, k, turn == 1)

            @pl.when(k < N_Z - 1)
            def _():
                dispatch_row(l, m, k, base)
            return carry
        lax.fori_loop(0, N_Z, sums_and_rows, 0)
        if m == 0:
            weights_wait(l)
        ffn(l, m, 0, base)
        finish(m_prev)
        if l_prev < n_layers - 1:
            gather_start(m_prev)

        def rest_ffn(k, carry):
            ffn(l, m, k, base + k)
            return carry
        lax.fori_loop(1, N_Z, rest_ffn, 0)
    l, m = turns[-1]

    def last_sums(k, carry):
        combine_step(l, m, k, False)
        return carry
    lax.fori_loop(0, N_Z, last_sums, 0)
    finish(m)

    results = [pltpu.make_async_copy(col.at[m, iz], out.at[m], load_sem.at[m, 0]) for m in range(n_micro)]
    for copy in results:
        copy.start()
    for slot in range(SEND_SLOTS):
        for r in range(1, N_PEER):
            d_copy(0, iz, slot, r).wait_send()
            r_copy(0, iz, slot, r).wait_send()
    for k in range(N_Z - 1):
        part_sent(0, row_of(k))
    for l in range(n_layers):
        for a in range(3):
            cross_copy(l, a).wait_send()
    for t in range(1, N_Z):
        table_copy(t).wait_send()
    for copy in results:
        copy.wait()


def solution(mesh):
    n_dev = mesh.shape["ez"] * mesh.shape["ey"] * mesh.shape["ex"]
    tok_spec = P(None, MESH_AXES, None)
    route_spec = P(None, None, MESH_AXES, None)
    weight_spec = P(None, MESH_AXES, None, None)

    def device_body(tokens_in, expert_ids, gate_vals, w_up1, w_up3, w_down):
        n_layers, n_micro, tok_mb, top_k = expert_ids.shape
        exp_dev = w_up1.shape[1]
        hidden, ffn_dim = w_up1.shape[2:]
        experts = exp_dev * n_dev
        capacity = capacity_of(tok_mb, top_k, experts)
        block = 2 * exp_dev * capacity
        slots = slot_table(expert_ids, experts, capacity)
        pad = ((0, 0), (0, 0), (0, 0), (0, 8 - top_k))
        routes = jnp.concatenate([jnp.pad(slots.astype(jnp.float32), pad), jnp.pad(gate_vals, pad)], axis=-1)
        routes = jnp.transpose(routes, (1, 0, 3, 2))
        vmem, any_space = pl.BlockSpec(memory_space=pltpu.VMEM), pl.BlockSpec(memory_space=pl.ANY)
        bf16, f32, dma = jnp.bfloat16, jnp.float32, pltpu.SemaphoreType.DMA
        rows_shape = jax.ShapeDtypeStruct((n_micro, N_Z, N_PEER, block, hidden), bf16)
        outs = pl.pallas_call(
            functools.partial(moe_kernel, capacity, top_k),
            in_specs=[any_space, vmem, any_space, any_space, any_space],
            out_specs=[any_space] * 7,
            out_shape=[
                jax.ShapeDtypeStruct(tokens_in.shape, bf16),
                rows_shape,
                rows_shape,
                jax.ShapeDtypeStruct((n_micro, 5, tok_mb, hidden), f32),
                jax.ShapeDtypeStruct(w_up1.shape, bf16),
                jax.ShapeDtypeStruct(w_up3.shape, bf16),
                jax.ShapeDtypeStruct(w_down.shape, bf16),
            ],
            scratch_shapes=[
                pltpu.VMEM((n_micro, N_Z, tok_mb, hidden), bf16),
                pltpu.VMEM((SEND_SLOTS, N_PEER, block, hidden), bf16),
                pltpu.VMEM((SEND_SLOTS, N_PEER, block, hidden), bf16),
                pltpu.VMEM((N_Z, tok_mb, hidden), f32),
                pltpu.VMEM((2 * exp_dev, hidden, ffn_dim), bf16),
                pltpu.VMEM((2 * exp_dev, hidden, ffn_dim), bf16),
                pltpu.VMEM((2 * exp_dev, ffn_dim, hidden), bf16),
                pltpu.VMEM((N_PEER, block, hidden), bf16),
                pltpu.VMEM((tok_mb, hidden), f32),
                pltpu.VMEM((tok_mb, N_PEER * block), bf16),
                pltpu.VMEM((tok_mb, N_PEER * block), bf16),
                pltpu.VMEM((N_Z,) + routes.shape, f32),
                dma((n_micro, N_Z - 1)),
                dma((n_micro, N_Z)),
                dma((SEND_SLOTS, N_PEER)),
                dma((n_micro, N_Z, N_PEER)),
                dma((SEND_SLOTS, N_PEER)),
                dma((n_micro, N_Z, N_PEER)),
                dma((N_Z,)),
                dma((n_micro, 5)),
                dma((n_layers, 3)),
                dma((n_layers, 3)),
                dma((N_Z - 1,)),
                dma((N_Z,)),
                dma((3, 2)),
                dma(()),
                dma(()),
            ],
            compiler_params=pltpu.CompilerParams(collective_id=0, has_side_effects=True, vmem_limit_bytes=VMEM_LIMIT),
            name="moe_layers",
        )(tokens_in, routes, w_up1, w_up3, w_down)
        return outs[0]

    return jax.shard_map(device_body, mesh=mesh, in_specs=(tok_spec, route_spec, route_spec, weight_spec, weight_spec, weight_spec), out_specs=tok_spec, check_vma=False)
```

```python
import functools

import jax
import jax.numpy as jnp
from jax import lax
from jax.experimental import pallas as pl
from jax.experimental.pallas import tpu as pltpu
from jax.sharding import PartitionSpec as P

ROUTE_SCALE = 2.5
MESH_AXES = ("ez", "ey", "ex")
N_Z = 4
N_PEER = 4
D_SLOTS = 6
R_SLOTS = 3
VMEM_LIMIT = 67043328
COLUMN = 512


def capacity_of(tok_mb, top_k, experts):
    return 2 * ((tok_mb * top_k + experts - 1) // experts)


def slot_table(ids, experts, capacity):
    chosen = (ids[..., None] == jnp.arange(experts)).astype(jnp.int32)
    per_expert = jnp.sum(chosen, axis=-2)
    token_rank = jnp.cumsum(per_expert, axis=-2) - per_expert
    slot_pos = jnp.sum(chosen * token_rank[..., None, :], axis=-1)
    return ids * capacity + slot_pos


def moe_kernel(capacity, top_k, tok_in, routes_in, w_up1, w_up3, w_down,
               out, d_land, r_land, c_land, x_up1, x_up3, x_down,
               col, d_buf, r_buf, part, v_up1, v_up3, v_down, stage, sum_stage, w_hi, w_lo, routes, routes_near,
               raw_send, raw_recv, ag_send, ag_recv, d_send, d_recv, r_send, r_recv, c_send, c_recv, x_send, x_recv,
               t_send, t_recv, n_send, n_recv, load_sem, copy_sem, self_sem):
    n_micro, n_layers = routes_in.shape[:2]
    tok_mb = routes_in.shape[3]
    hidden = col.shape[-1]
    exp_dev = w_up1.shape[1]
    block = d_buf.shape[2]
    column = min(COLUMN, hidden)
    iz, iy, ie = lax.axis_index("ez"), lax.axis_index("ey"), lax.axis_index("ex")
    ix, ic = ie // 2, ie % 2
    edge = jnp.minimum(iz, N_Z - 1 - iz)
    low = iz < N_Z // 2
    is_end = edge == 0
    is_mid = edge == 1
    mesh_id = pl.DeviceIdType.MESH

    def peer_chip(r):
        return (iy + r // 2) % 2, (ix + r % 2) % 2

    def peer(r, z=None):
        py, px = peer_chip(r)
        return (iz if z is None else z, py, px * 2 + ic)

    def near_axis(s):
        return 1 + s % 2

    def far_axis(s):
        return 2 - s % 2

    def relation(s, i):
        return (0, near_axis(s), far_axis(s), 3)[i]

    partner = (iz, iy, ix * 2 + (1 - ic))
    inner_z = jnp.where(low, jnp.where(is_end, 1, 2), jnp.where(is_end, 2, 1))
    outer_z = jnp.where(low, 0, N_Z - 1)

    def row_of(k):
        pos = jnp.where(k == 0, 3, jnp.where(k == 1, 2, jnp.where(k == 2, 1 - edge, edge)))
        return jnp.where(low, pos, N_Z - 1 - pos)

    def near_row(j):
        pos = jnp.where(j == 0, 1 - edge, j + 1)
        return jnp.where(low, pos, N_Z - 1 - pos)

    barrier = pltpu.get_barrier_semaphore()
    for r in range(1, N_PEER):
        pl.semaphore_signal(barrier, inc=1, device_id=peer(r), device_id_type=mesh_id)
    for t in range(1, N_Z):
        z = (iz + t) % N_Z
        pl.semaphore_signal(barrier, inc=1, device_id=peer(0, z), device_id_type=mesh_id)
        pl.semaphore_signal(barrier, inc=1, device_id=peer(near_axis(z), z), device_id_type=mesh_id)
    pl.semaphore_signal(barrier, inc=1, device_id=partner, device_id_type=mesh_id)
    pl.semaphore_wait(barrier, N_PEER + 2 * (N_Z - 1))

    def remote(src, dst, send_sem, recv_sem, device):
        return pltpu.make_async_remote_copy(src_ref=src, dst_ref=dst, send_sem=send_sem, recv_sem=recv_sem, device_id=device, device_id_type=mesh_id)

    def table_copy(t):
        return remote(routes_in, routes.at[iz], t_send.at[t - 1], t_recv.at[iz], peer(0, (iz + t) % N_Z))

    def near_table_copy(t):
        return remote(routes_in, routes_near.at[iz], n_send.at[t], n_recv.at[iz], peer(near_axis(iz), (iz + t) % N_Z))

    def tables_wait():
        for t in range(1, N_Z):
            z = (iz + t) % N_Z
            remote(routes_in, routes.at[z], t_send.at[0], t_recv.at[z], partner).wait_recv()
        for z in range(N_Z):
            remote(routes_in, routes_near.at[z], n_send.at[0], n_recv.at[z], partner).wait_recv()

    def gather_copy(m, t):
        return remote(col.at[m, 0, iz], col.at[m, 0, iz], ag_send.at[m, t - 1], ag_recv.at[m, iz], peer(0, (iz + t) % N_Z))

    def gather_wait(m, s):
        remote(col.at[m, 0, s], col.at[m, 0, s], ag_send.at[m, 0], ag_recv.at[m, s], partner).wait_recv()

    def raw_copy(m, s):
        return remote(col.at[m, 0, s], col.at[m, 1, s], raw_send.at[m, s], raw_recv.at[m, s], peer(near_axis(s)))

    def raw_sent(m):
        for z in range(N_Z):
            raw_copy(m, z).wait_send()

    def share(m):
        for t in (2, 1, 3):
            gather_copy(m, t).start()
        raw_copy(m, iz).start()

    def d_self(m, t, s, slot):
        return pltpu.make_async_copy(d_buf.at[slot, 0], d_land.at[m, s, t], self_sem)

    def d_copy(m, t, s, slot):
        return remote(d_buf.at[slot, 1], d_land.at[m, s, 2 + t], d_send.at[slot], d_recv.at[m, s, t], peer(far_axis(s)))

    def r_copy(m, s, slot, i):
        if i == 0:
            return pltpu.make_async_copy(r_buf.at[slot, 0], r_land.at[m, s, 0], self_sem)
        return remote(r_buf.at[slot, i], r_land.at[m, s, i], r_send.at[slot, i], r_recv.at[m, s, i], peer(relation(s, i)))

    def dispatch(l, m, t, s, count):
        slot = count % D_SLOTS

        @pl.when(count >= D_SLOTS)
        def _():
            d_copy(m, t, s, slot).wait_send()
        tokens = col[m, t, s]
        picks = (routes_near if t else routes)[s, m, l]
        row = lax.broadcasted_iota(jnp.int32, (block, tok_mb), 0)
        for dest in (1, 0):
            py, px = peer_chip(far_axis(s) if dest else 0)
            first = iz * (N_PEER * block) + (py * 2 + px) * block
            wanted = (row + first).astype(jnp.float32)
            hit = jnp.zeros((block, tok_mb), jnp.bool_)
            for k in range(top_k):
                hit = hit | (picks[k:k + 1, :] == wanted)
            pick = jnp.where(hit, 1.0, 0.0).astype(jnp.bfloat16)
            d_buf[slot, dest] = jnp.dot(pick, tokens, preferred_element_type=jnp.float32).astype(jnp.bfloat16)
            if dest:
                d_copy(m, t, s, slot).start()
        d_self(m, t, s, slot).start()
        d_self(m, t, s, slot).wait()

    def dispatch_held(l, m, s, count):
        dispatch(l, m, 0, s, count)

    def dispatch_arrived(l, m, j, count):
        s = near_row(j)
        gather_wait(m, s)
        raw_copy(m, s).start()
        dispatch_held(l, m, s, count + 1 + j)

    def dispatch_near(l, m, j, count):
        s = jnp.where(j == 0, iz, near_row(j - 1))
        raw_copy(m, s).wait_recv()
        dispatch(l, m, 1, s, count + N_Z + j)

    def ffn(l, m, k, count):
        s = row_of(k)
        slot = count % R_SLOTS
        for t in range(2):
            d_copy(m, t, s, 0).wait_recv()
        load = pltpu.make_async_copy(d_land.at[m, s], stage, copy_sem)
        load.start()

        @pl.when(count >= R_SLOTS)
        def _():
            for i in range(1, N_PEER):
                r_copy(m, s, slot, i).wait_send()
        load.wait()

        def one_expert(j, carry):
            at = pl.multiple_of(j * capacity, 16)
            rows = stage[:, pl.ds(at, capacity), :].reshape(N_PEER * capacity, hidden)
            gate_in = jnp.dot(rows, v_up1[j], preferred_element_type=jnp.float32)
            lin_in = jnp.dot(rows, v_up3[j], preferred_element_type=jnp.float32)
            act = (jax.nn.silu(gate_in) * lin_in).astype(jnp.bfloat16)
            res = jnp.dot(act, v_down[j], preferred_element_type=jnp.float32).astype(jnp.bfloat16)
            r_buf[slot, :, pl.ds(at, capacity), :] = res.reshape(N_PEER, capacity, hidden)
            return carry
        lax.fori_loop(0, 2 * exp_dev, one_expert, 0)
        for i in (3, 1, 2, 0):
            r_copy(m, s, slot, i).start()
        r_copy(m, s, slot, 0).wait()

    def chain_copy(m, s, kind, to_inner):
        return remote(part.at[s], c_land.at[m, kind], c_send.at[s], c_recv.at[m, kind], peer(0, inner_z if to_inner else outer_z))

    def chain_arrival(m, kind):
        remote(sum_stage, c_land.at[m, kind], c_send.at[0], c_recv.at[m, kind], partner).wait_recv()
        load = pltpu.make_async_copy(c_land.at[m, kind], sum_stage, copy_sem)
        load.start()
        load.wait()

    def part_sent(m, s):
        chain_copy(m, s, 0, True).wait_send()

    def combine(l, m, k, first):
        s = row_of(k)
        for i in range(1, N_PEER):
            r_copy(m, s, 0, i).wait_recv()
        load = pltpu.make_async_copy(r_land.at[m, s], stage, copy_sem)
        load.start()
        line = lax.broadcasted_iota(jnp.int32, (N_PEER * block, tok_mb), 0)
        target = line
        for i in range(N_PEER):
            py, px = peer_chip(relation(s, i))
            inside = (line >= i * block) & (line < (i + 1) * block)
            target = jnp.where(inside, line + (iz * (N_PEER * block) + (py * 2 + px - i) * block), target)
        target = target.astype(jnp.float32)
        table = routes[s, m, l]
        weight = jnp.zeros((N_PEER * block, tok_mb), jnp.float32)
        for j in range(top_k):
            weight = weight + jnp.where(table[j:j + 1, :] == target, table[8 + j:9 + j, :], 0.0)
        weight = weight.T
        high = weight.astype(jnp.bfloat16)
        w_hi[...] = high
        w_lo[...] = (weight - high.astype(jnp.float32)).astype(jnp.bfloat16)
        if not first:
            @pl.when(k < N_Z - 1)
            def _():
                part_sent(m, s)
        load.wait()

        def one_column(n, carry):
            cols = pl.ds(pl.multiple_of(n * column, column), column)
            rows = stage[:, :, cols].reshape(N_PEER * block, column)
            total = jnp.dot(w_hi[...], rows, preferred_element_type=jnp.float32)
            total = total + jnp.dot(w_lo[...], rows, preferred_element_type=jnp.float32)
            part[s, :, cols] = total
            return carry
        lax.fori_loop(0, hidden // column, one_column, 0)

        @pl.when(is_end & (k < N_Z - 1))
        def _():
            chain_copy(m, s, k, True).start()

    def forward(m, step):
        @pl.when(is_mid)
        def _():
            s = row_of(step)
            chain_arrival(m, (0, 1, 3)[step])
            part[s] = part[s] + sum_stage[...]
            chain_copy(m, s, (3, 4, 4)[step], step < 2).start()

    def combine_step(l, m, k, first):
        combine(l, m, k, first)
        for step in range(N_Z - 1):
            @pl.when(k == step + 1)
            def _():
                forward(m, step)

    def finish(m):
        for t in range(1, N_Z):
            gather_copy(m, t).wait_send()

        @pl.when(is_mid)
        def _():
            chain_arrival(m, 2)
            part[iz] = part[iz] + sum_stage[...]
        chain_arrival(m, 4)
        total = part[iz] + sum_stage[...]
        col[m, 0, iz] = (col[m, 0, iz].astype(jnp.float32) + ROUTE_SCALE * total).astype(jnp.bfloat16)

    sources = (w_up1, w_up3, w_down)
    crossed = (x_up1, x_up3, x_down)
    resident = (v_up1, v_up3, v_down)

    def cross_copy(l, a):
        return remote(sources[a].at[l], crossed[a].at[l], x_send.at[l, a], x_recv.at[l, a], partner)

    def weight_loads(l):
        own = [pltpu.make_async_copy(sources[a].at[l], resident[a].at[pl.ds(ic * exp_dev, exp_dev)], load_sem.at[a, 0]) for a in range(3)]
        other = [pltpu.make_async_copy(crossed[a].at[l], resident[a].at[pl.ds((1 - ic) * exp_dev, exp_dev)], load_sem.at[a, 1]) for a in range(3)]
        return own, other

    def weights_start(l):
        own, other = weight_loads(l)
        for copy in own:
            copy.start()
        for a in range(3):
            cross_copy(l, a).wait_recv()
            other[a].start()

    def weights_wait(l):
        own, other = weight_loads(l)
        for copy in own + other:
            copy.wait()

    first_load = [pltpu.make_async_copy(tok_in.at[m], col.at[m, 0, iz], load_sem.at[m, 0]) for m in range(n_micro)]
    for copy in first_load:
        copy.start()
    for t in range(1, N_Z):
        table_copy(t).start()
    for t in range(N_Z):
        near_table_copy(t).start()
    first_load[0].wait()
    share(0)
    for l in range(n_layers):
        for a in range(3):
            cross_copy(l, a).start()
    routes[iz] = routes_in[...]
    first_load[1].wait()
    tables_wait()
    dispatch_held(0, 0, iz, 0)
    share(1)

    def first_rows(j, carry):
        dispatch_near(0, 0, j, 0)

        @pl.when(j < N_Z - 1)
        def _():
            dispatch_arrived(0, 0, j, 0)
        return carry
    lax.fori_loop(0, N_Z, first_rows, 0)
    weights_start(0)
    weights_wait(0)

    def first_ffn(k, carry):
        ffn(0, 0, k, k)
        return carry
    lax.fori_loop(0, N_Z, first_ffn, 0)
    turns = [(l, m) for l in range(n_layers) for m in range(n_micro)]
    for turn in range(1, len(turns)):
        (l, m), (l_prev, m_prev) = turns[turn], turns[turn - 1]
        d_base, r_base = turn * 2 * N_Z, turn * N_Z
        raw_sent(m_prev)
        if m == 0:
            weights_start(l)
        dispatch_held(l, m, iz, d_base)

        def sums_and_rows(k, carry):
            combine_step(l_prev, m_prev, k, turn == 1)

            @pl.when(k < N_Z - 1)
            def _():
                dispatch_arrived(l, m, k, d_base)
            return carry
        lax.fori_loop(0, N_Z, sums_and_rows, 0)

        def near_rows(j, carry):
            dispatch_near(l, m, j, d_base)
            return carry
        lax.fori_loop(0, N_Z, near_rows, 0)
        finish(m_prev)
        if l_prev < n_layers - 1:
            share(m_prev)
        if m == 0:
            weights_wait(l)

        def turn_ffn(k, carry):
            ffn(l, m, k, r_base + k)
            return carry
        lax.fori_loop(0, N_Z, turn_ffn, 0)
    l, m = turns[-1]
    raw_sent(m)

    def last_sums(k, carry):
        combine_step(l, m, k, False)
        return carry
    lax.fori_loop(0, N_Z, last_sums, 0)
    finish(m)

    results = [pltpu.make_async_copy(col.at[m, 0, iz], out.at[m], load_sem.at[m, 0]) for m in range(n_micro)]
    for copy in results:
        copy.start()
    for slot in range(D_SLOTS):
        d_copy(0, 0, iz, slot).wait_send()
    for slot in range(R_SLOTS):
        for i in range(1, N_PEER):
            r_copy(0, iz, slot, i).wait_send()
    for k in range(N_Z - 1):
        part_sent(0, row_of(k))
    for l in range(n_layers):
        for a in range(3):
            cross_copy(l, a).wait_send()
    for t in range(1, N_Z):
        table_copy(t).wait_send()
    for t in range(N_Z):
        near_table_copy(t).wait_send()
    for copy in results:
        copy.wait()


def solution(mesh):
    n_dev = mesh.shape["ez"] * mesh.shape["ey"] * mesh.shape["ex"]
    tok_spec = P(None, MESH_AXES, None)
    route_spec = P(None, None, MESH_AXES, None)
    weight_spec = P(None, MESH_AXES, None, None)

    def device_body(tokens_in, expert_ids, gate_vals, w_up1, w_up3, w_down):
        n_layers, n_micro, tok_mb, top_k = expert_ids.shape
        exp_dev = w_up1.shape[1]
        hidden, ffn_dim = w_up1.shape[2:]
        experts = exp_dev * n_dev
        capacity = capacity_of(tok_mb, top_k, experts)
        block = 2 * exp_dev * capacity
        slots = slot_table(expert_ids, experts, capacity)
        pad = ((0, 0), (0, 0), (0, 0), (0, 8 - top_k))
        routes = jnp.concatenate([jnp.pad(slots.astype(jnp.float32), pad), jnp.pad(gate_vals, pad)], axis=-1)
        routes = jnp.transpose(routes, (1, 0, 3, 2))
        vmem, any_space = pl.BlockSpec(memory_space=pltpu.VMEM), pl.BlockSpec(memory_space=pl.ANY)
        bf16, f32, dma = jnp.bfloat16, jnp.float32, pltpu.SemaphoreType.DMA
        rows_shape = jax.ShapeDtypeStruct((n_micro, N_Z, N_PEER, block, hidden), bf16)
        outs = pl.pallas_call(
            functools.partial(moe_kernel, capacity, top_k),
            in_specs=[any_space, vmem, any_space, any_space, any_space],
            out_specs=[any_space] * 7,
            out_shape=[
                jax.ShapeDtypeStruct(tokens_in.shape, bf16),
                rows_shape,
                rows_shape,
                jax.ShapeDtypeStruct((n_micro, 5, tok_mb, hidden), f32),
                jax.ShapeDtypeStruct(w_up1.shape, bf16),
                jax.ShapeDtypeStruct(w_up3.shape, bf16),
                jax.ShapeDtypeStruct(w_down.shape, bf16),
            ],
            scratch_shapes=[
                pltpu.VMEM((n_micro, 2, N_Z, tok_mb, hidden), bf16),
                pltpu.VMEM((D_SLOTS, 2, block, hidden), bf16),
                pltpu.VMEM((R_SLOTS, N_PEER, block, hidden), bf16),
                pltpu.VMEM((N_Z, tok_mb, hidden), f32),
                pltpu.VMEM((2 * exp_dev, hidden, ffn_dim), bf16),
                pltpu.VMEM((2 * exp_dev, hidden, ffn_dim), bf16),
                pltpu.VMEM((2 * exp_dev, ffn_dim, hidden), bf16),
                pltpu.VMEM((N_PEER, block, hidden), bf16),
                pltpu.VMEM((tok_mb, hidden), f32),
                pltpu.VMEM((tok_mb, N_PEER * block), bf16),
                pltpu.VMEM((tok_mb, N_PEER * block), bf16),
                pltpu.VMEM((N_Z,) + routes.shape, f32),
                pltpu.VMEM((N_Z,) + routes.shape, f32),
                dma((n_micro, N_Z)),
                dma((n_micro, N_Z)),
                dma((n_micro, N_Z - 1)),
                dma((n_micro, N_Z)),
                dma((D_SLOTS,)),
                dma((n_micro, N_Z, 2)),
                dma((R_SLOTS, N_PEER)),
                dma((n_micro, N_Z, N_PEER)),
                dma((N_Z,)),
                dma((n_micro, 5)),
                dma((n_layers, 3)),
                dma((n_layers, 3)),
                dma((N_Z - 1,)),
                dma((N_Z,)),
                dma((N_Z,)),
                dma((N_Z,)),
                dma((3, 2)),
                dma(()),
                dma(()),
            ],
            compiler_params=pltpu.CompilerParams(collective_id=0, has_side_effects=True, vmem_limit_bytes=VMEM_LIMIT),
            name="moe_layers",
        )(tokens_in, routes, w_up1, w_up3, w_down)
        return outs[0]

    return jax.shard_map(device_body, mesh=mesh, in_specs=(tok_spec, route_spec, route_spec, weight_spec, weight_spec, weight_spec), out_specs=tok_spec, check_vma=False)
```

```python
import functools

import jax
import jax.numpy as jnp
from jax import lax
from jax.experimental import pallas as pl
from jax.experimental.pallas import tpu as pltpu
from jax.sharding import PartitionSpec as P

ROUTE_SCALE = 2.5
MESH_AXES = ("ez", "ey", "ex")
N_Z = 4
N_PEER = 4
D_SLOTS = 4
R_SLOTS = 4
VMEM_LIMIT = 67043328
COLUMN = 512


def capacity_of(tok_mb, top_k, experts):
    return 2 * ((tok_mb * top_k + experts - 1) // experts)


def slot_table(ids, experts, capacity):
    chosen = (ids[..., None] == jnp.arange(experts)).astype(jnp.int32)
    per_expert = jnp.sum(chosen, axis=-2)
    token_rank = jnp.cumsum(per_expert, axis=-2) - per_expert
    slot_pos = jnp.sum(chosen * token_rank[..., None, :], axis=-1)
    return ids * capacity + slot_pos


def moe_kernel(capacity, top_k, tok_in, routes_in, w_up1, w_up3, w_down,
               out, d_land, r_land, c_land, x_up1, x_up3, x_down,
               col, d_buf, r_buf, part, v_up1, v_up3, v_down, stage, sum_stage, w_hi, w_lo, routes, routes_near,
               raw_send, raw_recv, ag_send, ag_recv, d_send, d_recv, r_send, r_recv, c_send, c_recv, x_send, x_recv,
               t_send, t_recv, n_send, n_recv, load_sem, copy_sem, self_sem):
    n_micro, n_layers = routes_in.shape[:2]
    tok_mb = routes_in.shape[3]
    hidden = col.shape[-1]
    exp_dev = w_up1.shape[1]
    block = d_buf.shape[2]
    column = min(COLUMN, hidden)
    iz, iy, ie = lax.axis_index("ez"), lax.axis_index("ey"), lax.axis_index("ex")
    ix, ic = ie // 2, ie % 2
    edge = jnp.minimum(iz, N_Z - 1 - iz)
    low = iz < N_Z // 2
    is_end = edge == 0
    is_mid = edge == 1
    mesh_id = pl.DeviceIdType.MESH

    def peer_chip(r):
        return (iy + r // 2) % 2, (ix + r % 2) % 2

    def peer(r, z=None):
        py, px = peer_chip(r)
        return (iz if z is None else z, py, px * 2 + ic)

    def near_axis(s):
        return 1 + s % 2

    def far_axis(s):
        return 2 - s % 2

    def relation(s, i):
        return (0, near_axis(s), far_axis(s), 3)[i]

    partner = (iz, iy, ix * 2 + (1 - ic))
    inner_z = jnp.where(low, jnp.where(is_end, 1, 2), jnp.where(is_end, 2, 1))
    outer_z = jnp.where(low, 0, N_Z - 1)

    def row_of(k):
        pos = jnp.where(k == 0, 3, jnp.where(k == 1, 2, jnp.where(k == 2, 1 - edge, edge)))
        return jnp.where(low, pos, N_Z - 1 - pos)

    def near_row(j):
        pos = jnp.where(j == 0, 1 - edge, j + 1)
        return jnp.where(low, pos, N_Z - 1 - pos)

    barrier = pltpu.get_barrier_semaphore()
    for r in range(1, N_PEER):
        pl.semaphore_signal(barrier, inc=1, device_id=peer(r), device_id_type=mesh_id)
    for t in range(1, N_Z):
        z = (iz + t) % N_Z
        pl.semaphore_signal(barrier, inc=1, device_id=peer(0, z), device_id_type=mesh_id)
        pl.semaphore_signal(barrier, inc=1, device_id=peer(near_axis(z), z), device_id_type=mesh_id)
    pl.semaphore_signal(barrier, inc=1, device_id=partner, device_id_type=mesh_id)
    pl.semaphore_wait(barrier, N_PEER + 2 * (N_Z - 1))

    def remote(src, dst, send_sem, recv_sem, device):
        return pltpu.make_async_remote_copy(src_ref=src, dst_ref=dst, send_sem=send_sem, recv_sem=recv_sem, device_id=device, device_id_type=mesh_id)

    def table_copy(t):
        return remote(routes_in, routes.at[iz], t_send.at[t - 1], t_recv.at[iz], peer(0, (iz + t) % N_Z))

    def near_table_copy(t):
        return remote(routes_in, routes_near.at[iz], n_send.at[t], n_recv.at[iz], peer(near_axis(iz), (iz + t) % N_Z))

    def tables_wait():
        for t in range(1, N_Z):
            z = (iz + t) % N_Z
            remote(routes_in, routes.at[z], t_send.at[0], t_recv.at[z], partner).wait_recv()
        for z in range(N_Z):
            remote(routes_in, routes_near.at[z], n_send.at[0], n_recv.at[z], partner).wait_recv()

    def gather_copy(m, t):
        return remote(col.at[m, 0, iz], col.at[m, 0, iz], ag_send.at[m, t - 1], ag_recv.at[m, iz], peer(0, (iz + t) % N_Z))

    def gather_wait(m, s):
        remote(col.at[m, 0, s], col.at[m, 0, s], ag_send.at[m, 0], ag_recv.at[m, s], partner).wait_recv()

    def raw_copy(m, s):
        return remote(col.at[m, 0, s], col.at[m, 1, s], raw_send.at[m, s], raw_recv.at[m, s], peer(near_axis(s)))

    def raw_sent(m):
        for z in range(N_Z):
            raw_copy(m, z).wait_send()

    def share(m):
        for t in (2, 1, 3):
            gather_copy(m, t).start()
        raw_copy(m, iz).start()

    def d_self(m, t, s, slot):
        return pltpu.make_async_copy(d_buf.at[slot, 0], d_land.at[m, s, t], self_sem)

    def d_copy(m, t, s, slot):
        return remote(d_buf.at[slot, 1], d_land.at[m, s, 2 + t], d_send.at[slot], d_recv.at[m, s, t], peer(far_axis(s)))

    def r_copy(m, s, slot, i):
        if i == 0:
            return pltpu.make_async_copy(r_buf.at[slot, 0], r_land.at[m, s, 0], self_sem)
        return remote(r_buf.at[slot, i], r_land.at[m, s, i], r_send.at[slot, i], r_recv.at[m, s, i], peer(relation(s, i)))

    def dispatch(l, m, t, s, count):
        slot = count % D_SLOTS

        @pl.when(count >= D_SLOTS)
        def _():
            d_copy(m, t, s, slot).wait_send()
        tokens = col[m, t, s]
        picks = (routes_near if t else routes)[s, m, l]
        row = lax.broadcasted_iota(jnp.int32, (block, tok_mb), 0)
        for dest in (1, 0):
            py, px = peer_chip(far_axis(s) if dest else 0)
            first = iz * (N_PEER * block) + (py * 2 + px) * block
            wanted = (row + first).astype(jnp.float32)
            hit = jnp.zeros((block, tok_mb), jnp.bool_)
            for k in range(top_k):
                hit = hit | (picks[k:k + 1, :] == wanted)
            pick = jnp.where(hit, 1.0, 0.0).astype(jnp.bfloat16)
            d_buf[slot, dest] = jnp.dot(pick, tokens, preferred_element_type=jnp.float32).astype(jnp.bfloat16)
            if dest:
                d_copy(m, t, s, slot).start()
        d_self(m, t, s, slot).start()
        d_self(m, t, s, slot).wait()

    def dispatch_held(l, m, s, count):
        dispatch(l, m, 0, s, count)

    def dispatch_arrived(l, m, s, count):
        gather_wait(m, s)
        raw_copy(m, s).start()
        dispatch_held(l, m, s, count)

    def dispatch_near(l, m, s, count):
        raw_copy(m, s).wait_recv()
        dispatch(l, m, 1, s, count)

    def ffn(l, m, k, count):
        s = row_of(k)
        slot = count % R_SLOTS
        for t in range(2):
            d_copy(m, t, s, 0).wait_recv()
        load = pltpu.make_async_copy(d_land.at[m, s], stage, copy_sem)
        load.start()

        @pl.when(count >= R_SLOTS)
        def _():
            for i in range(1, N_PEER):
                r_copy(m, s, slot, i).wait_send()
        load.wait()

        def one_expert(j, carry):
            at = pl.multiple_of(j * capacity, 16)
            rows = stage[:, pl.ds(at, capacity), :].reshape(N_PEER * capacity, hidden)
            gate_in = jnp.dot(rows, v_up1[j], preferred_element_type=jnp.float32)
            lin_in = jnp.dot(rows, v_up3[j], preferred_element_type=jnp.float32)
            act = (jax.nn.silu(gate_in) * lin_in).astype(jnp.bfloat16)
            res = jnp.dot(act, v_down[j], preferred_element_type=jnp.float32).astype(jnp.bfloat16)
            r_buf[slot, :, pl.ds(at, capacity), :] = res.reshape(N_PEER, capacity, hidden)
            return carry
        lax.fori_loop(0, 2 * exp_dev, one_expert, 0)
        for i in (3, 1, 2, 0):
            r_copy(m, s, slot, i).start()
        r_copy(m, s, slot, 0).wait()

    def chain_copy(m, s, kind, to_inner):
        return remote(part.at[s], c_land.at[m, kind], c_send.at[s], c_recv.at[m, kind], peer(0, inner_z if to_inner else outer_z))

    def chain_arrival(m, kind):
        remote(sum_stage, c_land.at[m, kind], c_send.at[0], c_recv.at[m, kind], partner).wait_recv()
        load = pltpu.make_async_copy(c_land.at[m, kind], sum_stage, copy_sem)
        load.start()
        load.wait()

    def part_sent(m, s):
        chain_copy(m, s, 0, True).wait_send()

    def combine(l, m, k, first):
        s = row_of(k)
        for i in range(1, N_PEER):
            r_copy(m, s, 0, i).wait_recv()
        load = pltpu.make_async_copy(r_land.at[m, s], stage, copy_sem)
        load.start()
        line = lax.broadcasted_iota(jnp.int32, (N_PEER * block, tok_mb), 0)
        target = line
        for i in range(N_PEER):
            py, px = peer_chip(relation(s, i))
            inside = (line >= i * block) & (line < (i + 1) * block)
            target = jnp.where(inside, line + (iz * (N_PEER * block) + (py * 2 + px - i) * block), target)
        target = target.astype(jnp.float32)
        table = routes[s, m, l]
        weight = jnp.zeros((N_PEER * block, tok_mb), jnp.float32)
        for j in range(top_k):
            weight = weight + jnp.where(table[j:j + 1, :] == target, table[8 + j:9 + j, :], 0.0)
        weight = weight.T
        high = weight.astype(jnp.bfloat16)
        w_hi[...] = high
        w_lo[...] = (weight - high.astype(jnp.float32)).astype(jnp.bfloat16)
        if not first:
            @pl.when(k < N_Z - 1)
            def _():
                part_sent(m, s)
        load.wait()

        def one_column(n, carry):
            cols = pl.ds(pl.multiple_of(n * column, column), column)
            rows = stage[:, :, cols].reshape(N_PEER * block, column)
            total = jnp.dot(w_hi[...], rows, preferred_element_type=jnp.float32)
            total = total + jnp.dot(w_lo[...], rows, preferred_element_type=jnp.float32)
            part[s, :, cols] = total
            return carry
        lax.fori_loop(0, hidden // column, one_column, 0)

        @pl.when(is_end & (k < N_Z - 1))
        def _():
            chain_copy(m, s, k, True).start()

    def forward(m, step):
        @pl.when(is_mid)
        def _():
            s = row_of(step)
            chain_arrival(m, (0, 1, 3)[step])
            part[s] = part[s] + sum_stage[...]
            chain_copy(m, s, (3, 4, 4)[step], step < 2).start()

    def combine_step(l, m, k, first):
        combine(l, m, k, first)
        for step in range(N_Z - 1):
            @pl.when(k == step + 1)
            def _():
                forward(m, step)

    def finish(m):
        for t in range(1, N_Z):
            gather_copy(m, t).wait_send()

        @pl.when(is_mid)
        def _():
            chain_arrival(m, 2)
            part[iz] = part[iz] + sum_stage[...]
        chain_arrival(m, 4)
        total = part[iz] + sum_stage[...]
        col[m, 0, iz] = (col[m, 0, iz].astype(jnp.float32) + ROUTE_SCALE * total).astype(jnp.bfloat16)

    sources = (w_up1, w_up3, w_down)
    crossed = (x_up1, x_up3, x_down)
    resident = (v_up1, v_up3, v_down)

    def cross_copy(l, a):
        return remote(sources[a].at[l], crossed[a].at[l], x_send.at[l, a], x_recv.at[l, a], partner)

    def weight_loads(l):
        own = [pltpu.make_async_copy(sources[a].at[l], resident[a].at[pl.ds(ic * exp_dev, exp_dev)], load_sem.at[a, 0]) for a in range(3)]
        other = [pltpu.make_async_copy(crossed[a].at[l], resident[a].at[pl.ds((1 - ic) * exp_dev, exp_dev)], load_sem.at[a, 1]) for a in range(3)]
        return own, other

    def weights_start(l):
        own, other = weight_loads(l)
        for copy in own:
            copy.start()
        for a in range(3):
            cross_copy(l, a).wait_recv()
            other[a].start()

    def weights_wait(l):
        own, other = weight_loads(l)
        for copy in own + other:
            copy.wait()

    first_load = [pltpu.make_async_copy(tok_in.at[m], col.at[m, 0, iz], load_sem.at[m, 0]) for m in range(n_micro)]
    for copy in first_load:
        copy.start()
    for t in range(1, N_Z):
        table_copy(t).start()
    for t in range(N_Z):
        near_table_copy(t).start()
    first_load[0].wait()
    share(0)
    for l in range(n_layers):
        for a in range(3):
            cross_copy(l, a).start()
    routes[iz] = routes_in[...]
    first_load[1].wait()
    tables_wait()
    dispatch_held(0, 0, iz, 0)
    share(1)

    def first_rows(j, carry):
        dispatch_near(0, 0, jnp.where(j == 0, iz, near_row(j - 1)), 1 + 2 * j)

        @pl.when(j < N_Z - 1)
        def _():
            dispatch_arrived(0, 0, near_row(j), 2 + 2 * j)
        return carry
    lax.fori_loop(0, N_Z, first_rows, 0)
    weights_start(0)
    weights_wait(0)

    def first_ffn(k, carry):
        ffn(0, 0, k, k)
        return carry
    lax.fori_loop(0, N_Z, first_ffn, 0)
    turns = [(l, m) for l in range(n_layers) for m in range(n_micro)]
    for turn in range(1, len(turns)):
        (l, m), (l_prev, m_prev) = turns[turn], turns[turn - 1]
        d_base, r_base = turn * 2 * N_Z, turn * N_Z
        raw_sent(m_prev)
        if m == 0:
            weights_start(l)

        def sums_and_rows(k, carry):
            combine_step(l_prev, m_prev, k, turn == 1)

            @pl.when(k < N_Z - 1)
            def _():
                dispatch_arrived(l, m, row_of(k), d_base + k)
            return carry
        lax.fori_loop(0, N_Z, sums_and_rows, 0)
        dispatch_held(l, m, iz, d_base + N_Z - 1)

        def near_rows(j, carry):
            dispatch_near(l, m, row_of(j), d_base + N_Z + j)
            return carry
        lax.fori_loop(0, N_Z, near_rows, 0)
        finish(m_prev)
        if l_prev < n_layers - 1:
            share(m_prev)
        if m == 0:
            weights_wait(l)

        def turn_ffn(k, carry):
            ffn(l, m, k, r_base + k)
            return carry
        lax.fori_loop(0, N_Z, turn_ffn, 0)
    l, m = turns[-1]
    raw_sent(m)

    def last_sums(k, carry):
        combine_step(l, m, k, False)
        return carry
    lax.fori_loop(0, N_Z, last_sums, 0)
    finish(m)

    results = [pltpu.make_async_copy(col.at[m, 0, iz], out.at[m], load_sem.at[m, 0]) for m in range(n_micro)]
    for copy in results:
        copy.start()
    for slot in range(D_SLOTS):
        d_copy(0, 0, iz, slot).wait_send()
    for slot in range(R_SLOTS):
        for i in range(1, N_PEER):
            r_copy(0, iz, slot, i).wait_send()
    for k in range(N_Z - 1):
        part_sent(0, row_of(k))
    for l in range(n_layers):
        for a in range(3):
            cross_copy(l, a).wait_send()
    for t in range(1, N_Z):
        table_copy(t).wait_send()
    for t in range(N_Z):
        near_table_copy(t).wait_send()
    for copy in results:
        copy.wait()


def solution(mesh):
    n_dev = mesh.shape["ez"] * mesh.shape["ey"] * mesh.shape["ex"]
    tok_spec = P(None, MESH_AXES, None)
    route_spec = P(None, None, MESH_AXES, None)
    weight_spec = P(None, MESH_AXES, None, None)

    def device_body(tokens_in, expert_ids, gate_vals, w_up1, w_up3, w_down):
        n_layers, n_micro, tok_mb, top_k = expert_ids.shape
        exp_dev = w_up1.shape[1]
        hidden, ffn_dim = w_up1.shape[2:]
        experts = exp_dev * n_dev
        capacity = capacity_of(tok_mb, top_k, experts)
        block = 2 * exp_dev * capacity
        slots = slot_table(expert_ids, experts, capacity)
        pad = ((0, 0), (0, 0), (0, 0), (0, 8 - top_k))
        routes = jnp.concatenate([jnp.pad(slots.astype(jnp.float32), pad), jnp.pad(gate_vals, pad)], axis=-1)
        routes = jnp.transpose(routes, (1, 0, 3, 2))
        vmem, any_space = pl.BlockSpec(memory_space=pltpu.VMEM), pl.BlockSpec(memory_space=pl.ANY)
        bf16, f32, dma = jnp.bfloat16, jnp.float32, pltpu.SemaphoreType.DMA
        rows_shape = jax.ShapeDtypeStruct((n_micro, N_Z, N_PEER, block, hidden), bf16)
        outs = pl.pallas_call(
            functools.partial(moe_kernel, capacity, top_k),
            in_specs=[any_space, vmem, any_space, any_space, any_space],
            out_specs=[any_space] * 7,
            out_shape=[
                jax.ShapeDtypeStruct(tokens_in.shape, bf16),
                rows_shape,
                rows_shape,
                jax.ShapeDtypeStruct((n_micro, 5, tok_mb, hidden), f32),
                jax.ShapeDtypeStruct(w_up1.shape, bf16),
                jax.ShapeDtypeStruct(w_up3.shape, bf16),
                jax.ShapeDtypeStruct(w_down.shape, bf16),
            ],
            scratch_shapes=[
                pltpu.VMEM((n_micro, 2, N_Z, tok_mb, hidden), bf16),
                pltpu.VMEM((D_SLOTS, 2, block, hidden), bf16),
                pltpu.VMEM((R_SLOTS, N_PEER, block, hidden), bf16),
                pltpu.VMEM((N_Z, tok_mb, hidden), f32),
                pltpu.VMEM((2 * exp_dev, hidden, ffn_dim), bf16),
                pltpu.VMEM((2 * exp_dev, hidden, ffn_dim), bf16),
                pltpu.VMEM((2 * exp_dev, ffn_dim, hidden), bf16),
                pltpu.VMEM((N_PEER, block, hidden), bf16),
                pltpu.VMEM((tok_mb, hidden), f32),
                pltpu.VMEM((tok_mb, N_PEER * block), bf16),
                pltpu.VMEM((tok_mb, N_PEER * block), bf16),
                pltpu.VMEM((N_Z,) + routes.shape, f32),
                pltpu.VMEM((N_Z,) + routes.shape, f32),
                dma((n_micro, N_Z)),
                dma((n_micro, N_Z)),
                dma((n_micro, N_Z - 1)),
                dma((n_micro, N_Z)),
                dma((D_SLOTS,)),
                dma((n_micro, N_Z, 2)),
                dma((R_SLOTS, N_PEER)),
                dma((n_micro, N_Z, N_PEER)),
                dma((N_Z,)),
                dma((n_micro, 5)),
                dma((n_layers, 3)),
                dma((n_layers, 3)),
                dma((N_Z - 1,)),
                dma((N_Z,)),
                dma((N_Z,)),
                dma((N_Z,)),
                dma((3, 2)),
                dma(()),
                dma(()),
            ],
            compiler_params=pltpu.CompilerParams(collective_id=0, has_side_effects=True, vmem_limit_bytes=VMEM_LIMIT),
            name="moe_layers",
        )(tokens_in, routes, w_up1, w_up3, w_down)
        return outs[0]

    return jax.shard_map(device_body, mesh=mesh, in_specs=(tok_spec, route_spec, route_spec, weight_spec, weight_spec, weight_spec), out_specs=tok_spec, check_vma=False)
```

```python
import functools

import jax
import jax.numpy as jnp
from jax import lax
from jax.experimental import pallas as pl
from jax.experimental.pallas import tpu as pltpu
from jax.sharding import PartitionSpec as P

ROUTE_SCALE = 2.5
MESH_AXES = ("ez", "ey", "ex")
N_Z = 4
N_PEER = 4
D_SLOTS = 4
R_SLOTS = 4
VMEM_LIMIT = 67043328
COLUMN = 512


def capacity_of(tok_mb, top_k, experts):
    return 2 * ((tok_mb * top_k + experts - 1) // experts)


def slot_table(ids, experts, capacity):
    chosen = (ids[..., None] == jnp.arange(experts)).astype(jnp.int32)
    per_expert = jnp.sum(chosen, axis=-2)
    token_rank = jnp.cumsum(per_expert, axis=-2) - per_expert
    slot_pos = jnp.sum(chosen * token_rank[..., None, :], axis=-1)
    return ids * capacity + slot_pos


def moe_kernel(capacity, top_k, tok_in, routes_in, w_up1, w_up3, w_down,
               out, d_land, r_land, c_land, x_up1, x_up3, x_down,
               col, d_buf, r_buf, part, v_up1, v_up3, v_down, stage, sum_stage, w_hi, w_lo, routes, routes_near,
               raw_send, raw_recv, ag_send, ag_recv, d_send, d_recv, r_send, r_recv, c_send, c_recv, x_send, x_recv,
               t_send, t_recv, n_send, n_recv, load_sem, copy_sem, self_sem):
    n_micro, n_layers = routes_in.shape[:2]
    tok_mb = routes_in.shape[3]
    hidden = col.shape[-1]
    exp_dev = w_up1.shape[1]
    block = d_buf.shape[2]
    column = min(COLUMN, hidden)
    iz, iy, ie = lax.axis_index("ez"), lax.axis_index("ey"), lax.axis_index("ex")
    ix, ic = ie // 2, ie % 2
    edge = jnp.minimum(iz, N_Z - 1 - iz)
    low = iz < N_Z // 2
    is_end = edge == 0
    is_mid = edge == 1
    mesh_id = pl.DeviceIdType.MESH

    def peer_chip(r):
        return (iy + r // 2) % 2, (ix + r % 2) % 2

    def peer(r, z=None):
        py, px = peer_chip(r)
        return (iz if z is None else z, py, px * 2 + ic)

    def near_axis(s):
        return 1 + s % 2

    def far_axis(s):
        return 2 - s % 2

    def relation(s, i):
        return (0, near_axis(s), far_axis(s), 3)[i]

    partner = (iz, iy, ix * 2 + (1 - ic))
    inner_z = jnp.where(low, jnp.where(is_end, 1, 2), jnp.where(is_end, 2, 1))
    outer_z = jnp.where(low, 0, N_Z - 1)

    def row_of(k):
        pos = jnp.where(k == 0, 3, jnp.where(k == 1, 2, jnp.where(k == 2, 1 - edge, edge)))
        return jnp.where(low, pos, N_Z - 1 - pos)

    def near_row(j):
        pos = jnp.where(j == 0, 1 - edge, j + 1)
        return jnp.where(low, pos, N_Z - 1 - pos)

    barrier = pltpu.get_barrier_semaphore()
    for r in range(1, N_PEER):
        pl.semaphore_signal(barrier, inc=1, device_id=peer(r), device_id_type=mesh_id)
    for t in range(1, N_Z):
        z = (iz + t) % N_Z
        pl.semaphore_signal(barrier, inc=1, device_id=peer(0, z), device_id_type=mesh_id)
        pl.semaphore_signal(barrier, inc=1, device_id=peer(near_axis(z), z), device_id_type=mesh_id)
    pl.semaphore_signal(barrier, inc=1, device_id=partner, device_id_type=mesh_id)
    pl.semaphore_wait(barrier, N_PEER + 2 * (N_Z - 1))

    def remote(src, dst, send_sem, recv_sem, device):
        return pltpu.make_async_remote_copy(src_ref=src, dst_ref=dst, send_sem=send_sem, recv_sem=recv_sem, device_id=device, device_id_type=mesh_id)

    def table_copy(t):
        return remote(routes_in, routes.at[iz], t_send.at[t - 1], t_recv.at[iz], peer(0, (iz + t) % N_Z))

    def near_table_copy(t):
        return remote(routes_in, routes_near.at[iz], n_send.at[t], n_recv.at[iz], peer(near_axis(iz), (iz + t) % N_Z))

    def tables_wait():
        for t in range(1, N_Z):
            z = (iz + t) % N_Z
            remote(routes_in, routes.at[z], t_send.at[0], t_recv.at[z], partner).wait_recv()
        for z in range(N_Z):
            remote(routes_in, routes_near.at[z], n_send.at[0], n_recv.at[z], partner).wait_recv()

    def gather_copy(m, t):
        return remote(col.at[m, 0, iz], col.at[m, 0, iz], ag_send.at[m, t - 1], ag_recv.at[m, iz], peer(0, (iz + t) % N_Z))

    def gather_wait(m, s):
        remote(col.at[m, 0, s], col.at[m, 0, s], ag_send.at[m, 0], ag_recv.at[m, s], partner).wait_recv()

    def raw_copy(m, s):
        return remote(col.at[m, 0, s], col.at[m, 1, s], raw_send.at[m, s], raw_recv.at[m, s], peer(near_axis(s)))

    def raw_sent(m):
        for z in range(N_Z):
            raw_copy(m, z).wait_send()

    def share(m):
        for t in (2, 1, 3):
            gather_copy(m, t).start()
        raw_copy(m, iz).start()

    def d_self(m, t, s, slot):
        return pltpu.make_async_copy(d_buf.at[slot, 0], d_land.at[m, s, t], self_sem)

    def d_copy(m, t, s, slot):
        return remote(d_buf.at[slot, 1], d_land.at[m, s, 2 + t], d_send.at[slot], d_recv.at[m, s, t], peer(far_axis(s)))

    def r_copy(m, s, slot, i):
        if i == 0:
            return pltpu.make_async_copy(r_buf.at[slot, 0], r_land.at[m, s, 0], self_sem)
        return remote(r_buf.at[slot, i], r_land.at[m, s, i], r_send.at[slot, i], r_recv.at[m, s, i], peer(relation(s, i)))

    def dispatch(l, m, t, s, count):
        slot = count % D_SLOTS

        @pl.when(count >= D_SLOTS)
        def _():
            d_copy(m, t, s, slot).wait_send()
        tokens = col[m, t, s]
        picks = (routes_near if t else routes)[s, m, l]
        row = lax.broadcasted_iota(jnp.int32, (block, tok_mb), 0)
        for dest in (1, 0):
            py, px = peer_chip(far_axis(s) if dest else 0)
            first = iz * (N_PEER * block) + (py * 2 + px) * block
            wanted = (row + first).astype(jnp.float32)
            hit = jnp.zeros((block, tok_mb), jnp.bool_)
            for k in range(top_k):
                hit = hit | (picks[k:k + 1, :] == wanted)
            pick = jnp.where(hit, 1.0, 0.0).astype(jnp.bfloat16)
            d_buf[slot, dest] = jnp.dot(pick, tokens, preferred_element_type=jnp.float32).astype(jnp.bfloat16)
            if dest:
                d_copy(m, t, s, slot).start()

        @pl.when(count % (2 * N_Z) != 0)
        def _():
            d_self(m, t, s, slot).wait()
        d_self(m, t, s, slot).start()

    def dispatch_held(l, m, s, count):
        dispatch(l, m, 0, s, count)

    def dispatch_arrived(l, m, s, count):
        gather_wait(m, s)
        raw_copy(m, s).start()
        dispatch_held(l, m, s, count)

    def dispatch_near(l, m, s, count):
        raw_copy(m, s).wait_recv()
        dispatch(l, m, 1, s, count)

    def ffn(l, m, k, count):
        s = row_of(k)
        slot = count % R_SLOTS
        for t in range(2):
            d_copy(m, t, s, 0).wait_recv()
        load = pltpu.make_async_copy(d_land.at[m, s], stage, copy_sem)
        load.start()

        @pl.when(count >= R_SLOTS)
        def _():
            for i in range(1, N_PEER):
                r_copy(m, s, slot, i).wait_send()
        load.wait()

        def one_expert(j, carry):
            at = pl.multiple_of(j * capacity, 16)
            rows = stage[:, pl.ds(at, capacity), :].reshape(N_PEER * capacity, hidden)
            gate_in = jnp.dot(rows, v_up1[j], preferred_element_type=jnp.float32)
            lin_in = jnp.dot(rows, v_up3[j], preferred_element_type=jnp.float32)
            act = (jax.nn.silu(gate_in) * lin_in).astype(jnp.bfloat16)
            res = jnp.dot(act, v_down[j], preferred_element_type=jnp.float32).astype(jnp.bfloat16)
            r_buf[slot, :, pl.ds(at, capacity), :] = res.reshape(N_PEER, capacity, hidden)
            return carry
        lax.fori_loop(0, 2 * exp_dev, one_expert, 0)
        for i in (3, 1, 2, 0):
            if i == 0:
                @pl.when(k != 0)
                def _():
                    r_copy(m, s, slot, 0).wait()
            r_copy(m, s, slot, i).start()

    def chain_copy(m, s, kind, to_inner):
        return remote(part.at[s], c_land.at[m, kind], c_send.at[s], c_recv.at[m, kind], peer(0, inner_z if to_inner else outer_z))

    def chain_arrival(m, kind):
        remote(sum_stage, c_land.at[m, kind], c_send.at[0], c_recv.at[m, kind], partner).wait_recv()
        load = pltpu.make_async_copy(c_land.at[m, kind], sum_stage, copy_sem)
        load.start()
        load.wait()

    def part_sent(m, s):
        chain_copy(m, s, 0, True).wait_send()

    def combine(l, m, k, first):
        s = row_of(k)
        for i in range(1, N_PEER):
            r_copy(m, s, 0, i).wait_recv()
        load = pltpu.make_async_copy(r_land.at[m, s], stage, copy_sem)
        load.start()
        line = lax.broadcasted_iota(jnp.int32, (N_PEER * block, tok_mb), 0)
        target = line
        for i in range(N_PEER):
            py, px = peer_chip(relation(s, i))
            inside = (line >= i * block) & (line < (i + 1) * block)
            target = jnp.where(inside, line + (iz * (N_PEER * block) + (py * 2 + px - i) * block), target)
        target = target.astype(jnp.float32)
        table = routes[s, m, l]
        weight = jnp.zeros((N_PEER * block, tok_mb), jnp.float32)
        for j in range(top_k):
            weight = weight + jnp.where(table[j:j + 1, :] == target, table[8 + j:9 + j, :], 0.0)
        weight = weight.T
        high = weight.astype(jnp.bfloat16)
        w_hi[...] = high
        w_lo[...] = (weight - high.astype(jnp.float32)).astype(jnp.bfloat16)
        if not first:
            @pl.when(k < N_Z - 1)
            def _():
                part_sent(m, s)
        load.wait()

        def one_column(n, carry):
            cols = pl.ds(pl.multiple_of(n * column, column), column)
            rows = stage[:, :, cols].reshape(N_PEER * block, column)
            total = jnp.dot(w_hi[...], rows, preferred_element_type=jnp.float32)
            total = total + jnp.dot(w_lo[...], rows, preferred_element_type=jnp.float32)
            part[s, :, cols] = total
            return carry
        lax.fori_loop(0, hidden // column, one_column, 0)

        @pl.when(is_end & (k < N_Z - 1))
        def _():
            chain_copy(m, s, k, True).start()

    def forward(m, step):
        @pl.when(is_mid)
        def _():
            s = row_of(step)
            chain_arrival(m, (0, 1, 3)[step])
            part[s] = part[s] + sum_stage[...]
            chain_copy(m, s, (3, 4, 4)[step], step < 2).start()

    def combine_step(l, m, k, first):
        combine(l, m, k, first)
        for step in range(N_Z - 1):
            @pl.when(k == step + 1)
            def _():
                forward(m, step)

    def finish(m):
        for t in range(1, N_Z):
            gather_copy(m, t).wait_send()

        @pl.when(is_mid)
        def _():
            chain_arrival(m, 2)
            part[iz] = part[iz] + sum_stage[...]
        chain_arrival(m, 4)
        total = part[iz] + sum_stage[...]
        col[m, 0, iz] = (col[m, 0, iz].astype(jnp.float32) + ROUTE_SCALE * total).astype(jnp.bfloat16)

    sources = (w_up1, w_up3, w_down)
    crossed = (x_up1, x_up3, x_down)
    resident = (v_up1, v_up3, v_down)

    def cross_copy(l, a):
        return remote(sources[a].at[l], crossed[a].at[l], x_send.at[l, a], x_recv.at[l, a], partner)

    def weight_loads(l):
        own = [pltpu.make_async_copy(sources[a].at[l], resident[a].at[pl.ds(ic * exp_dev, exp_dev)], load_sem.at[a, 0]) for a in range(3)]
        other = [pltpu.make_async_copy(crossed[a].at[l], resident[a].at[pl.ds((1 - ic) * exp_dev, exp_dev)], load_sem.at[a, 1]) for a in range(3)]
        return own, other

    def weights_start(l):
        own, other = weight_loads(l)
        for copy in own:
            copy.start()
        for a in range(3):
            cross_copy(l, a).wait_recv()
            other[a].start()

    def weights_wait(l):
        own, other = weight_loads(l)
        for copy in own + other:
            copy.wait()

    first_load = [pltpu.make_async_copy(tok_in.at[m], col.at[m, 0, iz], load_sem.at[m, 0]) for m in range(n_micro)]
    for copy in first_load:
        copy.start()
    for t in range(1, N_Z):
        table_copy(t).start()
    for t in range(N_Z):
        near_table_copy(t).start()
    first_load[0].wait()
    share(0)
    for l in range(n_layers):
        for a in range(3):
            cross_copy(l, a).start()
    routes[iz] = routes_in[...]
    first_load[1].wait()
    tables_wait()
    dispatch_held(0, 0, iz, 0)
    share(1)

    def first_rows(j, carry):
        dispatch_near(0, 0, jnp.where(j == 0, iz, near_row(j - 1)), 1 + 2 * j)

        @pl.when(j < N_Z - 1)
        def _():
            dispatch_arrived(0, 0, near_row(j), 2 + 2 * j)
        return carry
    lax.fori_loop(0, N_Z, first_rows, 0)
    d_self(0, 0, iz, 0).wait()
    weights_start(0)
    weights_wait(0)

    def first_ffn(k, carry):
        ffn(0, 0, k, k)
        return carry
    lax.fori_loop(0, N_Z, first_ffn, 0)
    r_copy(0, iz, 0, 0).wait()
    turns = [(l, m) for l in range(n_layers) for m in range(n_micro)]
    for turn in range(1, len(turns)):
        (l, m), (l_prev, m_prev) = turns[turn], turns[turn - 1]
        d_base, r_base = turn * 2 * N_Z, turn * N_Z
        raw_sent(m_prev)
        if m == 0:
            weights_start(l)

        def sums_and_rows(k, carry):
            combine_step(l_prev, m_prev, k, turn == 1)

            @pl.when(k < N_Z - 1)
            def _():
                dispatch_arrived(l, m, row_of(k), d_base + k)
            return carry
        lax.fori_loop(0, N_Z, sums_and_rows, 0)
        dispatch_held(l, m, iz, d_base + N_Z - 1)

        def near_rows(j, carry):
            dispatch_near(l, m, row_of(j), d_base + N_Z + j)
            return carry
        lax.fori_loop(0, N_Z, near_rows, 0)
        d_self(m, 0, iz, 0).wait()
        finish(m_prev)
        if l_prev < n_layers - 1:
            share(m_prev)
        if m == 0:
            weights_wait(l)

        def turn_ffn(k, carry):
            ffn(l, m, k, r_base + k)
            return carry
        lax.fori_loop(0, N_Z, turn_ffn, 0)
        r_copy(m, iz, 0, 0).wait()
    l, m = turns[-1]
    raw_sent(m)

    def last_sums(k, carry):
        combine_step(l, m, k, False)
        return carry
    lax.fori_loop(0, N_Z, last_sums, 0)
    finish(m)

    results = [pltpu.make_async_copy(col.at[m, 0, iz], out.at[m], load_sem.at[m, 0]) for m in range(n_micro)]
    for copy in results:
        copy.start()
    for slot in range(D_SLOTS):
        d_copy(0, 0, iz, slot).wait_send()
    for slot in range(R_SLOTS):
        for i in range(1, N_PEER):
            r_copy(0, iz, slot, i).wait_send()
    for k in range(N_Z - 1):
        part_sent(0, row_of(k))
    for l in range(n_layers):
        for a in range(3):
            cross_copy(l, a).wait_send()
    for t in range(1, N_Z):
        table_copy(t).wait_send()
    for t in range(N_Z):
        near_table_copy(t).wait_send()
    for copy in results:
        copy.wait()


def solution(mesh):
    n_dev = mesh.shape["ez"] * mesh.shape["ey"] * mesh.shape["ex"]
    tok_spec = P(None, MESH_AXES, None)
    route_spec = P(None, None, MESH_AXES, None)
    weight_spec = P(None, MESH_AXES, None, None)

    def device_body(tokens_in, expert_ids, gate_vals, w_up1, w_up3, w_down):
        n_layers, n_micro, tok_mb, top_k = expert_ids.shape
        exp_dev = w_up1.shape[1]
        hidden, ffn_dim = w_up1.shape[2:]
        experts = exp_dev * n_dev
        capacity = capacity_of(tok_mb, top_k, experts)
        block = 2 * exp_dev * capacity
        slots = slot_table(expert_ids, experts, capacity)
        pad = ((0, 0), (0, 0), (0, 0), (0, 8 - top_k))
        routes = jnp.concatenate([jnp.pad(slots.astype(jnp.float32), pad), jnp.pad(gate_vals, pad)], axis=-1)
        routes = jnp.transpose(routes, (1, 0, 3, 2))
        vmem, any_space = pl.BlockSpec(memory_space=pltpu.VMEM), pl.BlockSpec(memory_space=pl.ANY)
        bf16, f32, dma = jnp.bfloat16, jnp.float32, pltpu.SemaphoreType.DMA
        rows_shape = jax.ShapeDtypeStruct((n_micro, N_Z, N_PEER, block, hidden), bf16)
        outs = pl.pallas_call(
            functools.partial(moe_kernel, capacity, top_k),
            in_specs=[any_space, vmem, any_space, any_space, any_space],
            out_specs=[any_space] * 7,
            out_shape=[
                jax.ShapeDtypeStruct(tokens_in.shape, bf16),
                rows_shape,
                rows_shape,
                jax.ShapeDtypeStruct((n_micro, 5, tok_mb, hidden), f32),
                jax.ShapeDtypeStruct(w_up1.shape, bf16),
                jax.ShapeDtypeStruct(w_up3.shape, bf16),
                jax.ShapeDtypeStruct(w_down.shape, bf16),
            ],
            scratch_shapes=[
                pltpu.VMEM((n_micro, 2, N_Z, tok_mb, hidden), bf16),
                pltpu.VMEM((D_SLOTS, 2, block, hidden), bf16),
                pltpu.VMEM((R_SLOTS, N_PEER, block, hidden), bf16),
                pltpu.VMEM((N_Z, tok_mb, hidden), f32),
                pltpu.VMEM((2 * exp_dev, hidden, ffn_dim), bf16),
                pltpu.VMEM((2 * exp_dev, hidden, ffn_dim), bf16),
                pltpu.VMEM((2 * exp_dev, ffn_dim, hidden), bf16),
                pltpu.VMEM((N_PEER, block, hidden), bf16),
                pltpu.VMEM((tok_mb, hidden), f32),
                pltpu.VMEM((tok_mb, N_PEER * block), bf16),
                pltpu.VMEM((tok_mb, N_PEER * block), bf16),
                pltpu.VMEM((N_Z,) + routes.shape, f32),
                pltpu.VMEM((N_Z,) + routes.shape, f32),
                dma((n_micro, N_Z)),
                dma((n_micro, N_Z)),
                dma((n_micro, N_Z - 1)),
                dma((n_micro, N_Z)),
                dma((D_SLOTS,)),
                dma((n_micro, N_Z, 2)),
                dma((R_SLOTS, N_PEER)),
                dma((n_micro, N_Z, N_PEER)),
                dma((N_Z,)),
                dma((n_micro, 5)),
                dma((n_layers, 3)),
                dma((n_layers, 3)),
                dma((N_Z - 1,)),
                dma((N_Z,)),
                dma((N_Z,)),
                dma((N_Z,)),
                dma((3, 2)),
                dma(()),
                dma(()),
            ],
            compiler_params=pltpu.CompilerParams(collective_id=0, has_side_effects=True, vmem_limit_bytes=VMEM_LIMIT),
            name="moe_layers",
        )(tokens_in, routes, w_up1, w_up3, w_down)
        return outs[0]

    return jax.shard_map(device_body, mesh=mesh, in_specs=(tok_spec, route_spec, route_spec, weight_spec, weight_spec, weight_spec), out_specs=tok_spec, check_vma=False)
```
